128 devices in a mesh: seq: 16 (over z, x), head: 8 (over y, core).
Axes of the slice: x: 4, y: 4, z: 4, core: 2. Of those that a mesh axis runs over, the one named last changes fastest.
Arguments:
- context: bfloat16 [32768, 2048], P('seq'), may hold values from -64 to 64
- wq_cross: bfloat16 [2048, 2048], P(None, 'head'), may hold values from -4 to 4
- wk_cross: bfloat16 [2048, 2048], P(None, 'head'), may hold values from -4 to 4
- wv_cross: bfloat16 [2048, 2048], P(None, 'head'), may hold values from -0.125 to 0.125
- wo_cross: bfloat16 [2048, 2048], P('head'), may hold values from -0.125 to 0.125
- wq_latent: bfloat16 [2048, 2048], P(None, 'head'), may hold values from -4 to 4
- wk_latent: bfloat16 [2048, 2048], P(None, 'head'), may hold values from -4 to 4
- wv_latent: bfloat16 [2048, 2048], P(None, 'head'), may hold values from -0.125 to 0.125
- wo_latent: bfloat16 [2048, 2048], P('head'), may hold values from -0.125 to 0.125
- cross_keep: int32 [16, 2048, 4096], P('head', None, 'seq'), may hold values from 0 to 255, as said below
- latent_keep: int32 [16, 2048, 128], P('head'), may hold values from 0 to 65535, as said below
- residual_keep: int32 [2, 2048, 128], replicated, may hold values from 0 to 65535, as said below
Outputs:
- latents_out: bfloat16 [2048, 2048], P('seq', 'head')
The draws below stay inside these ranges and needn't reach their ends.
Inputs may be any that keep to these rules, and one draw needn't show every extreme that they name: `cross_keep`: each of the 8 low bits of a word is one keep flag, laid out as the steps say. `latent_keep`: each of the 16 low bits of a word is one keep flag, laid out as the steps say. `residual_keep`: each of the 16 low bits of a word is one keep flag, laid out as the steps say.
All inputs are finite; a program needn't handle non-finite values.
Results may differ from the reference program's by a relative error of at most 0.015.
Values may be sent and summed in bfloat16 or wider, within the bound.
No kernel may reach another device: no remote copies, remote signals or barrier semaphores. Data moves between devices by JAX's collectives and lax.ppermute only.
A program may use at most 128 MiB of HBM per device.

```python
import math
import jax
import jax.numpy as jnp
from jax import lax

D = 2048
HEADS = 16
HEAD_DIM = 128
NL = 2048
TOKENS = 32768
N_SEQ = 16


def draw_context(key, part):
    columns = jnp.arange(D, dtype=jnp.float32) / max(D - 1, 1)
    row_scale = jnp.exp(jax.random.uniform(jax.random.fold_in(key, 301), (TOKENS, 1), jnp.float32, jnp.log(0.3), jnp.log(3.0)))
    base_draw = jnp.clip(jax.random.normal(jax.random.fold_in(key, 303), (TOKENS, D), jnp.float32), -4.5, 4.5)
    column_ramp = 10.0 ** (columns - 0.5)
    return (base_draw * column_ramp[None, :] * row_scale).astype(jnp.bfloat16)


def score_weight(key, pair_index, side_index):
    model_width = HEADS * HEAD_DIM
    own_part = jnp.clip(jax.random.normal(jax.random.fold_in(key, 400 + 10 * pair_index + side_index), (D, model_width), jnp.float32), -4.5, 4.5)
    entries = 1.7 * own_part
    return (entries / jnp.sqrt(D * 1.0)).astype(jnp.bfloat16)


def draw_wq_cross(key, part):
    return score_weight(key, 0, 0)


def draw_wk_cross(key, part):
    return score_weight(key, 0, 1)


def draw_wq_latent(key, part):
    return score_weight(key, 1, 0)


def draw_wk_latent(key, part):
    return score_weight(key, 1, 1)


def keep_words(key, salt_value, shape, word_bits):
    highest = 2 ** word_bits
    first = jax.random.randint(jax.random.fold_in(key, salt_value), shape, 0, highest, dtype=jnp.int32)
    second = jax.random.randint(jax.random.fold_in(key, salt_value + 1), shape, 0, highest, dtype=jnp.int32)
    third = jax.random.randint(jax.random.fold_in(key, salt_value + 2), shape, 0, highest, dtype=jnp.int32)
    return first | second | third


def draw_cross_keep(key, part):
    return keep_words(key, 500, (HEADS, NL, TOKENS // 8), 8)


def draw_latent_keep(key, part):
    return keep_words(key, 600, (HEADS, NL, NL // 16), 16)


def draw_residual_keep(key, part):
    return keep_words(key, 700, (2, NL, D // 16), 16)


def steps_of(stream_key, extent, split, low, top_value):
    gain, own = 1.0, jax.random.fold_in(stream_key, 6)
    for position, blocks in split:
        draws = jnp.exp(jax.random.uniform(jax.random.fold_in(own, position), (blocks,), jnp.float32, low / len(split), top_value / len(split)))
        gain = gain * jnp.repeat(draws, extent[position] // blocks).reshape([-1 if axis == position else 1 for axis in range(len(extent))])
    return gain


def bell_draw(stream_key, shape, spread, reach, shards=(), kind=jnp.bfloat16):
    values = jax.random.normal(stream_key, shape, jnp.float32) * spread
    if len(shards) > 0:
        values = steps_of(stream_key, shape, shards, -0.22, 0.18) * values
    return jnp.clip(values, min=-reach, max=reach).astype(kind)


def setup_inputs(seed: int = 0) -> dict:
    splits = jax.random.split(jax.random.key(seed), 13)
    return {
        "context": draw_context(jax.random.fold_in(splits[12], 71), 0),
        "wq_cross": draw_wq_cross(jax.random.fold_in(splits[12], 71), 0),
        "wk_cross": draw_wk_cross(jax.random.fold_in(splits[12], 71), 0),
        "wv_cross": bell_draw(splits[3], (D, HEADS * HEAD_DIM), D ** -0.5, 0.125, ((1, 8),)),
        "wo_cross": bell_draw(splits[4], (HEADS * HEAD_DIM, D), (HEADS * HEAD_DIM) ** -0.5, 0.125, ((0, 8),)),
        "wq_latent": draw_wq_latent(jax.random.fold_in(splits[12], 71), 0),
        "wk_latent": draw_wk_latent(jax.random.fold_in(splits[12], 71), 0),
        "wv_latent": bell_draw(splits[7], (D, HEADS * HEAD_DIM), D ** -0.5, 0.125, ((1, 8),)),
        "wo_latent": bell_draw(splits[8], (HEADS * HEAD_DIM, D), (HEADS * HEAD_DIM) ** -0.5, 0.125, ((0, 8),)),
        "cross_keep": draw_cross_keep(jax.random.fold_in(splits[12], 71), 0),
        "latent_keep": draw_latent_keep(jax.random.fold_in(splits[12], 71), 0),
        "residual_keep": draw_residual_keep(jax.random.fold_in(splits[12], 71), 0),
    }


keep_scale = 8.0 / 7.0

def unpack_bits(packed_words, word_bits):
    shifts = jnp.arange(word_bits, dtype=jnp.int32)
    bit_table = jnp.bitwise_and(jnp.right_shift(packed_words[..., None, :], shifts[:, None]), 1)
    return bit_table.reshape(packed_words.shape[:-1] + (word_bits * packed_words.shape[-1],))

def rms_rows(matrix):
    wide_rows = matrix.astype(jnp.float32)
    mean_square = lax.optimization_barrier(jnp.mean(wide_rows * wide_rows, axis=-1, keepdims=True))
    return (wide_rows * lax.rsqrt(mean_square + 1e-06)).astype(jnp.bfloat16)

def split_heads(matrix):
    return matrix.reshape(matrix.shape[0], HEADS, HEAD_DIM).transpose(1, 0, 2)

def join_heads(stacked):
    return stacked.transpose(1, 0, 2).reshape(stacked.shape[1], HEADS * HEAD_DIM).astype(jnp.bfloat16)

def attend(queries, key_rows, value_rows, packed, groups, word_bits, query_pos, key_pos):
    score_scale = 1.0 / math.sqrt(HEAD_DIM)

    def one_head(head_items):
        query_rows, head_keys, head_values, packed_words = head_items
        scores = jnp.dot(query_rows, head_keys.T, preferred_element_type=jnp.float32) * score_scale
        allowed = key_pos[None, :] <= query_pos[:, None]
        scores = jnp.where(allowed, scores, -1e+30)
        row_top = lax.optimization_barrier(jnp.max(scores, axis=-1, keepdims=True))
        exponent = jnp.where(allowed, jnp.exp(scores - row_top), 0.0)
        row_sum = lax.optimization_barrier(jnp.sum(exponent, axis=-1, keepdims=True))
        grouped = packed_words.reshape(packed_words.shape[0], groups, -1)
        keep_flags = unpack_bits(grouped, word_bits).reshape(packed_words.shape[0], -1).astype(jnp.float32)
        weights = (exponent / row_sum * keep_flags * keep_scale).astype(jnp.bfloat16)
        return jnp.dot(weights, head_values, preferred_element_type=jnp.float32)
    return lax.map(one_head, (queries, key_rows, value_rows, packed))

def reference(context, wq_cross, wk_cross, wv_cross, wo_cross, wq_latent, wk_latent, wv_latent, wo_latent, cross_keep, latent_keep, residual_keep):
    first_latent = TOKENS - NL
    normed = rms_rows(context)
    key_rows = jnp.dot(normed, wk_cross, preferred_element_type=jnp.float32).astype(jnp.bfloat16)
    value_rows = jnp.dot(normed, wv_cross, preferred_element_type=jnp.float32).astype(jnp.bfloat16)
    queries = jnp.dot(normed[first_latent:], wq_cross, preferred_element_type=jnp.float32).astype(jnp.bfloat16)
    latent_pos = jnp.arange(NL, dtype=jnp.int32)
    context_pos = jnp.arange(TOKENS, dtype=jnp.int32)
    attended = join_heads(attend(split_heads(queries), split_heads(key_rows), split_heads(value_rows), cross_keep, N_SEQ, 8, first_latent + latent_pos, context_pos))
    residual_flags = unpack_bits(residual_keep, 16).astype(jnp.float32)
    branch = jnp.dot(attended, wo_cross, preferred_element_type=jnp.float32)
    latents = (context[first_latent:].astype(jnp.float32) + residual_flags[0] * keep_scale * branch).astype(jnp.bfloat16)
    normed_latents = rms_rows(latents)
    latent_queries = jnp.dot(normed_latents, wq_latent, preferred_element_type=jnp.float32).astype(jnp.bfloat16)
    latent_keys = jnp.dot(normed_latents, wk_latent, preferred_element_type=jnp.float32).astype(jnp.bfloat16)
    latent_values = jnp.dot(normed_latents, wv_latent, preferred_element_type=jnp.float32).astype(jnp.bfloat16)
    latent_attended = join_heads(attend(split_heads(latent_queries), split_heads(latent_keys), split_heads(latent_values), latent_keep, 1, 16, latent_pos, latent_pos))
    latent_branch = jnp.dot(latent_attended, wo_latent, preferred_element_type=jnp.float32)
    return (latents.astype(jnp.float32) + residual_flags[1] * keep_scale * latent_branch).astype(jnp.bfloat16)
```

```python
import math

import jax
import jax.numpy as jnp
from jax import lax
from jax.experimental import pallas as pl
from jax.experimental.pallas import tpu as pltpu
from jax.sharding import PartitionSpec as P


bf16 = jnp.bfloat16
f32 = jnp.float32
keep_scale = 8.0 / 7.0
masked = -1e30
head_dim = 128
query_scale = math.log2(math.e) / math.sqrt(head_dim)
stat_rows = 16


def params(limit=48):
    return pltpu.CompilerParams(
        dimension_semantics=("arbitrary",), vmem_limit_bytes=limit * 1024 * 1024
    )


def row_scale(rows):
    wide = rows.astype(f32)
    mean_square = jnp.mean(wide * wide, axis=-1, keepdims=True)
    return lax.rsqrt(mean_square + 1e-06)


def query_kernel(chunks, per_step, root, where_ref, x_ref, own_ref, w_ref, *out_refs):
    step = pl.program_id(0)
    rows = chunks

    @pl.when(where_ref[0] == root)
    def _():
        x = x_ref[...]
        product = jnp.dot(x, w_ref[...], preferred_element_type=f32)
        scaled = (product * (row_scale(x) * query_scale)).astype(bf16)
        for k, out_ref in enumerate(out_refs):

            @pl.when(step == k // per_step)
            def _():
                first = (k % per_step) * rows
                out_ref[:, :256] = scaled[first : first + rows]
                out_ref[:, 256:] = own_ref[first : first + rows, :]


def query_chunks(where, context, wq, seq_count):
    tok_rows, width = context.shape
    columns = wq.shape[1]
    rows = tok_rows // seq_count
    per_step = 2
    block = rows * per_step
    root = seq_count - 1
    grid = (tok_rows // block,)
    spec = pltpu.PrefetchScalarGridSpec(
        num_scalar_prefetch=1,
        grid=grid,
        in_specs=[
            pl.BlockSpec((block, width), lambda i, at: (jnp.where(at[0] == root, i, 0), 0)),
            pl.BlockSpec((block, columns), lambda i, at: (jnp.where(at[0] == root, i, 0), at[1])),
            pl.BlockSpec((width, columns), lambda i, at: (0, 0)),
        ],
        out_specs=[pl.BlockSpec((rows, 2 * columns), lambda i, at: (0, 0))] * seq_count,
    )
    return pl.pallas_call(
        lambda *refs: query_kernel(rows, per_step, root, *refs),
        grid_spec=spec,
        out_shape=[jax.ShapeDtypeStruct((rows, 2 * columns), bf16)] * seq_count,
        compiler_params=params(),
        name="queries",
    )(where, context, context, wq)


def kv_kernel(x_ref, wk_ref, wv_ref, k_ref, v_ref):
    x = x_ref[...]
    scale = row_scale(x)
    k_ref[...] = (jnp.dot(x, wk_ref[...], preferred_element_type=f32) * scale).astype(bf16)
    v_ref[...] = (jnp.dot(x, wv_ref[...], preferred_element_type=f32) * scale).astype(bf16)


def keys_values(context, wk, wv):
    tok_rows, width = context.shape
    columns = wk.shape[1]
    block = 256
    return pl.pallas_call(
        kv_kernel,
        grid=(tok_rows // block,),
        in_specs=[
            pl.BlockSpec((block, width), lambda i: (i, 0)),
            pl.BlockSpec((width, columns), lambda i: (0, 0)),
            pl.BlockSpec((width, columns), lambda i: (0, 0)),
        ],
        out_specs=[pl.BlockSpec((block, columns), lambda i: (i, 0))] * 2,
        out_shape=[jax.ShapeDtypeStruct((tok_rows, columns), bf16)] * 2,
        compiler_params=params(),
        name="keys_values",
    )(context, wk, wv)


def softmax_rows(scores_of, keep_of, values_of, pieces):
    scores = [scores_of(b) for b in range(pieces)]
    top = scores[0]
    for s in scores[1:]:
        top = jnp.maximum(top, s)
    top = jnp.max(top, axis=-1, keepdims=True)
    total = None
    summed = None
    for b in range(pieces):
        p = jnp.exp2(scores[b] - top)
        total = p if total is None else total + p
        kept = jnp.where(keep_of(b), p, 0.0).astype(bf16)
        part = jnp.dot(kept, values_of(b), preferred_element_type=f32)
        summed = part if summed is None else summed + part
    total = jnp.sum(total, axis=-1, keepdims=True)
    return summed, top, total


def nt_dot(a, b):
    return lax.dot_general(a, b, (((1,), (1,)), ((), ())), preferred_element_type=f32)


def cross_kernel(root, where_ref, q_ref, k_ref, v_ref, words_ref, out_ref):
    rows = q_ref.shape[1]
    step = pl.program_id(0)

    def run(causal):
        lanes = lax.broadcasted_iota(jnp.int32, (rows, head_dim), 1)
        stats = jnp.zeros((rows, head_dim), f32)
        for head in range(2):
            cols = slice(head * head_dim, (head + 1) * head_dim)
            q = q_ref[0, :, cols]
            words = words_ref[head]
            wide = words.shape[1]

            def scores_of(b):
                s = nt_dot(q, k_ref[b * wide : (b + 1) * wide, cols])
                if causal:
                    key = b * wide + lax.broadcasted_iota(jnp.int32, s.shape, 1)
                    row = step * rows + lax.broadcasted_iota(jnp.int32, s.shape, 0)
                    s = jnp.where(key <= row, s, masked)
                return s

            summed, top, total = softmax_rows(
                scores_of,
                lambda b: (words & (1 << b)) != 0,
                lambda b: v_ref[b * wide : (b + 1) * wide, cols],
                8,
            )
            out_ref[0, head * rows : (head + 1) * rows, :] = (
                summed * (keep_scale / total)
            ).astype(bf16)
            lse = top + jnp.log2(total)
            high = lse.astype(bf16).astype(f32)
            middle = (lse - high).astype(bf16).astype(f32)
            low = lse - high - middle
            for n, piece in enumerate((high, middle, low)):
                stats = jnp.where(lanes == head * 3 + n, piece, stats)
        out_ref[0, 2 * rows :, :] = stats.T[:stat_rows].astype(bf16)

    @pl.when(where_ref[0] == root)
    def _():
        run(True)

    @pl.when(where_ref[0] != root)
    def _():
        run(False)


def cross_attention(where, queries, keys, values, words, root):
    count, rows, _ = queries.shape
    spec = pltpu.PrefetchScalarGridSpec(
        num_scalar_prefetch=1,
        grid=(count,),
        in_specs=[
            pl.BlockSpec((1, rows, 256), lambda i, at: (i, 0, 0)),
            pl.BlockSpec(keys.shape, lambda i, at: (0, 0)),
            pl.BlockSpec(values.shape, lambda i, at: (0, 0)),
            pl.BlockSpec((2, rows, words.shape[2]), lambda i, at: (0, i, 0)),
        ],
        out_specs=pl.BlockSpec((1, 2 * rows + stat_rows, head_dim), lambda i, at: (i, 0, 0)),
    )
    return pl.pallas_call(
        lambda *refs: cross_kernel(root, *refs),
        grid_spec=spec,
        out_shape=jax.ShapeDtypeStruct((count, 2 * rows + stat_rows, head_dim), bf16),
        compiler_params=params(),
        name="cross_attention",
    )(where, queries, keys, values, words)


def combine_kernel(parts_ref, wo_ref, out_ref):
    count = parts_ref.shape[0]
    rows = head_dim
    heads = []
    stats = parts_ref[:, 2 * rows :, :].astype(f32)
    for head in range(2):
        lse = stats[:, head * 3] + stats[:, head * 3 + 1] + stats[:, head * 3 + 2]
        weight = jnp.exp2(lse - jnp.max(lse, axis=0, keepdims=True))
        weight = weight / jnp.sum(weight, axis=0, keepdims=True)
        weight = jnp.concatenate([weight, jnp.zeros((rows - count, rows), f32)], axis=0).T
        mixed = None
        for s in range(count):
            part = parts_ref[s, head * rows : (head + 1) * rows, :].astype(f32)
            part = part * weight[:, s : s + 1]
            mixed = part if mixed is None else mixed + part
        heads.append(mixed.astype(bf16))
    attended = jnp.concatenate(heads, axis=1)
    for h in range(out_ref.shape[0]):
        out_ref[h] = jnp.dot(
            attended, wo_ref[:, h * 256 : (h + 1) * 256], preferred_element_type=f32
        ).astype(bf16)


def combine(parts, wo, head_count):
    return pl.pallas_call(
        combine_kernel,
        out_shape=jax.ShapeDtypeStruct((head_count, head_dim, 256), bf16),
        compiler_params=pltpu.CompilerParams(vmem_limit_bytes=48 * 1024 * 1024),
        name="combine",
    )(parts, wo)


def residual_kernel(index, where_ref, parts_ref, base_ref, words_ref, out_ref):
    total = parts_ref[0].astype(f32)
    for h in range(1, parts_ref.shape[0]):
        total = total + parts_ref[h].astype(f32)
    words = words_ref[0]
    for half in range(2):
        cols = slice(half * 128, half * 128 + 128)
        flag = (jnp.right_shift(words, where_ref[1] * 2 + half) & 1).astype(f32)
        base = base_ref[:, cols].astype(f32)
        out_ref[:, cols] = (base + flag * keep_scale * total[:, cols]).astype(bf16)


def residual(where, parts, base, base_block, words, index):
    count, rows, columns = parts.shape
    spec = pltpu.PrefetchScalarGridSpec(
        num_scalar_prefetch=1,
        grid=(1,),
        in_specs=[
            pl.BlockSpec(parts.shape, lambda i, at: (0, 0, 0)),
            pl.BlockSpec((rows, columns), lambda i, at: (0, base_block)),
            pl.BlockSpec((1, rows, 128), lambda i, at: (index, at[0], 0)),
        ],
        out_specs=pl.BlockSpec((rows, columns), lambda i, at: (0, 0)),
    )
    return pl.pallas_call(
        lambda *refs: residual_kernel(index, *refs),
        grid_spec=spec,
        out_shape=jax.ShapeDtypeStruct((rows, columns), bf16),
        compiler_params=params(),
        name="residual",
    )(where, parts, base, words)


def latent_qkv_kernel(x_ref, wq_ref, wk_ref, wv_ref, q_ref, kv_ref):
    count, rows, columns = x_ref.shape
    squares = None
    for h in range(count):
        wide = x_ref[h].astype(f32)
        part = jnp.sum(wide * wide, axis=-1, keepdims=True)
        squares = part if squares is None else squares + part
    scale = lax.rsqrt(squares / (count * columns) + 1e-06)

    def project(w_ref):
        total = None
        for h in range(count):
            part = jnp.dot(
                x_ref[h], w_ref[h * columns : (h + 1) * columns, :], preferred_element_type=f32
            )
            total = part if total is None else total + part
        return total * scale

    q_ref[...] = (project(wq_ref) * query_scale).astype(bf16)
    keys = project(wk_ref).astype(bf16)
    values = project(wv_ref).astype(bf16)
    for s in range(kv_ref.shape[0]):
        kv_ref[s, :, :columns] = keys
        kv_ref[s, :, columns:] = values


def latent_qkv(latents, wq, wk, wv, seq_count):
    count, rows, columns = latents.shape
    return pl.pallas_call(
        latent_qkv_kernel,
        out_shape=[
            jax.ShapeDtypeStruct((rows, columns), bf16),
            jax.ShapeDtypeStruct((seq_count, rows, 2 * columns), bf16),
        ],
        compiler_params=pltpu.CompilerParams(vmem_limit_bytes=48 * 1024 * 1024),
        name="latent_qkv",
    )(latents, wq, wk, wv)


def latent_kernel(where_ref, q_ref, kv_ref, words_ref, wo_ref, out_ref):
    count, rows, _ = kv_ref.shape
    heads = []
    for head in range(2):
        cols = slice(head * head_dim, (head + 1) * head_dim)
        value_cols = slice(256 + head * head_dim, 256 + (head + 1) * head_dim)
        q = q_ref[:, cols]
        words = words_ref[head]

        def scores_of(t):
            s = nt_dot(q, kv_ref[t, :, cols])
            key = t * rows + lax.broadcasted_iota(jnp.int32, s.shape, 1)
            row = where_ref[0] * rows + lax.broadcasted_iota(jnp.int32, s.shape, 0)
            return jnp.where(key <= row, s, masked)

        summed, top, total = softmax_rows(
            scores_of,
            lambda t: (words & (1 << t)) != 0,
            lambda t: kv_ref[t, :, value_cols],
            count,
        )
        heads.append((summed * (keep_scale / total)).astype(bf16))
    attended = jnp.concatenate(heads, axis=1)
    for h in range(out_ref.shape[0]):
        out_ref[h] = jnp.dot(
            attended, wo_ref[:, h * 256 : (h + 1) * 256], preferred_element_type=f32
        ).astype(bf16)


def latent_attention(where, q, kv, words, wo, head_count):
    rows, columns = q.shape
    spec = pltpu.PrefetchScalarGridSpec(
        num_scalar_prefetch=1,
        grid=(1,),
        in_specs=[
            pl.BlockSpec(q.shape, lambda i, at: (0, 0)),
            pl.BlockSpec(kv.shape, lambda i, at: (0, 0, 0)),
            pl.BlockSpec((2, rows, 128), lambda i, at: (0, at[0], 0)),
            pl.BlockSpec(wo.shape, lambda i, at: (0, 0)),
        ],
        out_specs=pl.BlockSpec((head_count, rows, columns), lambda i, at: (0, 0, 0)),
    )
    return pl.pallas_call(
        latent_kernel,
        grid_spec=spec,
        out_shape=jax.ShapeDtypeStruct((head_count, rows, columns), bf16),
        compiler_params=params(),
        name="latent_attention",
    )(where, q, kv, words, wo)


def exchange(value, axis):
    return lax.all_to_all(value, axis, 0, 0, tiled=True)


def per_device(
    context,
    wq_cross,
    wk_cross,
    wv_cross,
    wo_cross,
    wq_latent,
    wk_latent,
    wv_latent,
    wo_latent,
    cross_keep,
    latent_keep,
    residual_keep,
):
    seq_count = lax.axis_size("seq")
    head_count = lax.axis_size("head")
    root = seq_count - 1
    seq_index = lax.axis_index("seq").astype(jnp.int32)
    head_index = lax.axis_index("head").astype(jnp.int32)
    where = jnp.stack([seq_index, head_index])

    chunks = query_chunks(where, context, wq_cross, seq_count)
    mine = chunks[root]
    for k in range(root):
        got = lax.ppermute(chunks[k], "seq", [(root, k)])
        mine = jnp.where(seq_index == k, got, mine)
    keys, values = keys_values(context, wk_cross, wv_cross)
    own_queries = mine[:, :256]
    queries = exchange(
        jnp.broadcast_to(own_queries[None], (seq_count, *own_queries.shape)), "seq"
    )
    parts = cross_attention(where, queries, keys, values, cross_keep, root)
    parts = exchange(parts, "seq")
    branch = combine(parts, wo_cross, head_count)
    branch = exchange(branch, "head")
    latents = residual(where, branch, mine, 1, residual_keep, 0)
    all_columns = lax.all_gather(latents, "head", axis=0, tiled=False)
    q, kv = latent_qkv(all_columns, wq_latent, wk_latent, wv_latent, seq_count)
    kv = exchange(kv, "seq")
    branch = latent_attention(where, q, kv, latent_keep, wo_latent, head_count)
    branch = exchange(branch, "head")
    return residual(where, branch, latents, 0, residual_keep, 1)


def solution(mesh):
    in_specs = (
        P("seq", None),
        P(None, "head"),
        P(None, "head"),
        P(None, "head"),
        P("head", None),
        P(None, "head"),
        P(None, "head"),
        P(None, "head"),
        P("head", None),
        P("head", None, "seq"),
        P("head", None, None),
        P(),
    )
    out_specs = P("seq", "head")
    return jax.shard_map(
        per_device, mesh=mesh, in_specs=in_specs, out_specs=out_specs, check_vma=False
    )
```

```python
import math

import jax
import jax.numpy as jnp
from jax import lax
from jax.experimental import pallas as pl
from jax.experimental.pallas import tpu as pltpu
from jax.sharding import PartitionSpec as P


bf16 = jnp.bfloat16
f32 = jnp.float32
keep_scale = 8.0 / 7.0
masked = -1e30
head_dim = 128
query_scale = math.log2(math.e) / math.sqrt(head_dim)
stat_rows = 16


def params(limit=48):
    return pltpu.CompilerParams(
        dimension_semantics=("arbitrary",), vmem_limit_bytes=limit * 1024 * 1024
    )


def row_scale(rows):
    wide = rows.astype(f32)
    mean_square = jnp.mean(wide * wide, axis=-1, keepdims=True)
    return lax.rsqrt(mean_square + 1e-06)


def query_kernel(root, where_ref, x_ref, w_ref, out_ref):
    @pl.when(where_ref[0] == root)
    def _():
        x = x_ref[...]
        product = jnp.dot(x, w_ref[...], preferred_element_type=f32)
        out_ref[...] = (
            (product * (row_scale(x) * query_scale)).astype(bf16).reshape(out_ref.shape)
        )


def query_chunks(where, context, wq, seq_count):
    tok_rows, width = context.shape
    columns = wq.shape[1]
    rows = tok_rows // seq_count
    group = 4
    root = seq_count - 1
    spec = pltpu.PrefetchScalarGridSpec(
        num_scalar_prefetch=1,
        grid=(seq_count // group,),
        in_specs=[
            pl.BlockSpec((rows * group, width), lambda i, at: (jnp.where(at[0] == root, i, 0), 0)),
            pl.BlockSpec((width, columns), lambda i, at: (0, 0)),
        ],
        out_specs=pl.BlockSpec((group, rows, columns), lambda i, at: (i, 0, 0)),
    )
    return pl.pallas_call(
        lambda *refs: query_kernel(root, *refs),
        grid_spec=spec,
        out_shape=jax.ShapeDtypeStruct((seq_count, rows, columns), bf16),
        compiler_params=params(52),
        name="queries",
    )(where, context, wq)


def kv_kernel(x_ref, wk_ref, wv_ref, k_ref, v_ref):
    x = x_ref[...]
    scale = row_scale(x)
    k_ref[...] = (jnp.dot(x, wk_ref[...], preferred_element_type=f32) * scale).astype(bf16)
    v_ref[...] = (jnp.dot(x, wv_ref[...], preferred_element_type=f32) * scale).astype(bf16)


def keys_values(context, wk, wv):
    tok_rows, width = context.shape
    columns = wk.shape[1]
    block = 512
    return pl.pallas_call(
        kv_kernel,
        grid=(tok_rows // block,),
        in_specs=[
            pl.BlockSpec((block, width), lambda i: (i, 0)),
            pl.BlockSpec((width, columns), lambda i: (0, 0)),
            pl.BlockSpec((width, columns), lambda i: (0, 0)),
        ],
        out_specs=[pl.BlockSpec((block, columns), lambda i: (i, 0))] * 2,
        out_shape=[jax.ShapeDtypeStruct((tok_rows, columns), bf16)] * 2,
        compiler_params=params(52),
        name="keys_values",
    )(context, wk, wv)


def softmax_rows(scores_of, keep_of, values_of, pieces):
    scores = [scores_of(b) for b in range(pieces)]
    top = scores[0]
    for s in scores[1:]:
        top = jnp.maximum(top, s)
    top = jnp.max(top, axis=-1, keepdims=True)
    total = None
    summed = None
    for b in range(pieces):
        p = jnp.exp2(scores[b] - top)
        total = p if total is None else total + p
        kept = jnp.where(keep_of(b), p, 0.0).astype(bf16)
        part = jnp.dot(kept, values_of(b), preferred_element_type=f32)
        summed = part if summed is None else summed + part
    total = jnp.sum(total, axis=-1, keepdims=True)
    return summed, top, total


def nt_dot(a, b):
    return lax.dot_general(a, b, (((1,), (1,)), ((), ())), preferred_element_type=f32)


def cross_kernel(root, n, where_ref, q_ref, k_ref, v_ref, words_ref, out_ref, s0_ref, s1_ref, m_ref):
    rows = n * head_dim
    wide = words_ref.shape[2]
    step = pl.program_id(0)
    following = jnp.minimum(step + 1, pl.num_programs(0) - 1)

    def run(causal):
        def score(head, block, b):
            cols = slice(head * head_dim, (head + 1) * head_dim)
            q = q_ref[pl.ds(block * n, n), :, cols].reshape(rows, head_dim)
            s = nt_dot(q, k_ref[b * wide : (b + 1) * wide, cols])
            if causal:
                key = b * wide + lax.broadcasted_iota(jnp.int32, s.shape, 1)
                row = block * rows + lax.broadcasted_iota(jnp.int32, s.shape, 0)
                s = jnp.where(key <= row, s, masked)
            return s

        def stage(head, next_block):
            ready, filling = (s0_ref, s1_ref) if head == 0 else (s1_ref, s0_ref)
            cols = slice(head * head_dim, (head + 1) * head_dim)
            words = words_ref[head].astype(jnp.int16)
            top = jnp.max(m_ref[head], axis=-1, keepdims=True)
            total = None
            summed = None
            next_top = None
            for b in range(8):
                s = score(1 - head, next_block, b)
                p = jnp.exp2(ready[b] - top)
                total = p if total is None else total + p
                kept = jnp.where((words & jnp.int16(1 << b)) != jnp.int16(0), p.astype(bf16), bf16(0))
                part = jnp.dot(
                    kept, v_ref[b * wide : (b + 1) * wide, cols], preferred_element_type=f32
                )
                summed = part if summed is None else summed + part
                filling[b] = s
                next_top = s if next_top is None else jnp.maximum(next_top, s)
            m_ref[1 - head] = next_top
            total = jnp.sum(total, axis=-1, keepdims=True)
            out = (summed * (keep_scale / total)).astype(bf16)
            for i in range(n):
                out_ref[i, head * head_dim : (head + 1) * head_dim, :] = out[
                    i * head_dim : (i + 1) * head_dim
                ]
            return top + jnp.log2(total)

        @pl.when(step == 0)
        def _():
            first_top = None
            for b in range(8):
                s = score(0, 0, b)
                s0_ref[b] = s
                first_top = s if first_top is None else jnp.maximum(first_top, s)
            m_ref[0] = first_top

        sums = [stage(0, step), stage(1, following)]
        lanes = lax.broadcasted_iota(jnp.int32, (rows, head_dim), 1)
        stats = jnp.zeros((rows, head_dim), f32)
        for head, lse in enumerate(sums):
            high = lse.astype(bf16).astype(f32)
            middle = (lse - high).astype(bf16).astype(f32)
            low = lse - high - middle
            for j, piece in enumerate((high, middle, low)):
                stats = jnp.where(lanes == head * 3 + j, piece, stats)
        for i in range(n):
            out_ref[i, 2 * head_dim :, :] = (
                stats[i * head_dim : (i + 1) * head_dim].T[:stat_rows].astype(bf16)
            )

    @pl.when(where_ref[0] == root)
    def _():
        run(True)

    @pl.when(where_ref[0] != root)
    def _():
        run(False)


def cross_attention(where, queries, keys, values, words, root):
    count = queries.shape[0]
    n = 4
    rows = n * head_dim
    wide = words.shape[2]
    whole = pl.Buffered(1)
    spec = pltpu.PrefetchScalarGridSpec(
        num_scalar_prefetch=1,
        grid=(count // n,),
        in_specs=[
            pl.BlockSpec(queries.shape, lambda i, at: (0, 0, 0), pipeline_mode=whole),
            pl.BlockSpec(keys.shape, lambda i, at: (0, 0), pipeline_mode=whole),
            pl.BlockSpec(values.shape, lambda i, at: (0, 0), pipeline_mode=whole),
            pl.BlockSpec((2, rows, wide), lambda i, at: (0, i, 0)),
        ],
        out_specs=pl.BlockSpec((n, 2 * head_dim + stat_rows, head_dim), lambda i, at: (i, 0, 0)),
        scratch_shapes=[
            pltpu.VMEM((8, rows, wide), f32),
            pltpu.VMEM((8, rows, wide), f32),
            pltpu.VMEM((2, rows, wide), f32),
        ],
    )
    return pl.pallas_call(
        lambda *refs: cross_kernel(root, n, *refs),
        grid_spec=spec,
        out_shape=jax.ShapeDtypeStruct((count, 2 * head_dim + stat_rows, head_dim), bf16),
        compiler_params=params(52),
        name="cross_attention",
    )(where, queries, keys, values, words)


def combine_kernel(parts_ref, wo_ref, out_ref):
    count = parts_ref.shape[0]
    rows = head_dim
    heads = []
    stats = parts_ref[:, 2 * rows :, :].astype(f32)
    for head in range(2):
        lse = stats[:, head * 3] + stats[:, head * 3 + 1] + stats[:, head * 3 + 2]
        weight = jnp.exp2(lse - jnp.max(lse, axis=0, keepdims=True))
        weight = weight / jnp.sum(weight, axis=0, keepdims=True)
        weight = jnp.concatenate([weight, jnp.zeros((rows - count, rows), f32)], axis=0).T
        mixed = None
        for s in range(count):
            part = parts_ref[s, head * rows : (head + 1) * rows, :].astype(f32)
            part = part * weight[:, s : s + 1]
            mixed = part if mixed is None else mixed + part
        heads.append(mixed.astype(bf16))
    attended = jnp.concatenate(heads, axis=1)
    for h in range(out_ref.shape[0]):
        out_ref[h] = jnp.dot(
            attended, wo_ref[:, h * 256 : (h + 1) * 256], preferred_element_type=f32
        ).astype(bf16)


def combine(parts, wo, head_count):
    return pl.pallas_call(
        combine_kernel,
        out_shape=jax.ShapeDtypeStruct((head_count, head_dim, 256), bf16),
        compiler_params=pltpu.CompilerParams(vmem_limit_bytes=48 * 1024 * 1024),
        name="combine",
    )(parts, wo)


def residual_kernel(index, where_ref, parts_ref, base_ref, words_ref, out_ref):
    total = parts_ref[0].astype(f32)
    for h in range(1, parts_ref.shape[0]):
        total = total + parts_ref[h].astype(f32)
    words = words_ref[0]
    for half in range(2):
        cols = slice(half * 128, half * 128 + 128)
        flag = (jnp.right_shift(words, where_ref[1] * 2 + half) & 1).astype(f32)
        base = base_ref[:, cols].astype(f32)
        out_ref[:, cols] = (base + flag * keep_scale * total[:, cols]).astype(bf16)


def residual(where, parts, base, base_block, words, index):
    count, rows, columns = parts.shape
    spec = pltpu.PrefetchScalarGridSpec(
        num_scalar_prefetch=1,
        grid=(1,),
        in_specs=[
            pl.BlockSpec(parts.shape, lambda i, at: (0, 0, 0)),
            pl.BlockSpec((rows, columns), lambda i, at: (0, base_block)),
            pl.BlockSpec((1, rows, 128), lambda i, at: (index, at[0], 0)),
        ],
        out_specs=pl.BlockSpec((rows, columns), lambda i, at: (0, 0)),
    )
    return pl.pallas_call(
        lambda *refs: residual_kernel(index, *refs),
        grid_spec=spec,
        out_shape=jax.ShapeDtypeStruct((rows, columns), bf16),
        compiler_params=params(),
        name="residual",
    )(where, parts, base, words)


def latent_qkv_kernel(x_ref, wq_ref, wk_ref, wv_ref, q_ref, kv_ref):
    count, rows, columns = x_ref.shape
    squares = None
    for h in range(count):
        wide = x_ref[h].astype(f32)
        part = jnp.sum(wide * wide, axis=-1, keepdims=True)
        squares = part if squares is None else squares + part
    scale = lax.rsqrt(squares / (count * columns) + 1e-06)

    def project(w_ref):
        total = None
        for h in range(count):
            part = jnp.dot(
                x_ref[h], w_ref[h * columns : (h + 1) * columns, :], preferred_element_type=f32
            )
            total = part if total is None else total + part
        return total * scale

    q_ref[...] = (project(wq_ref) * query_scale).astype(bf16)
    keys = project(wk_ref).astype(bf16)
    values = project(wv_ref).astype(bf16)
    for s in range(kv_ref.shape[0]):
        kv_ref[s, :, :columns] = keys
        kv_ref[s, :, columns:] = values


def latent_qkv(latents, wq, wk, wv, seq_count):
    count, rows, columns = latents.shape
    return pl.pallas_call(
        latent_qkv_kernel,
        out_shape=[
            jax.ShapeDtypeStruct((rows, columns), bf16),
            jax.ShapeDtypeStruct((seq_count, rows, 2 * columns), bf16),
        ],
        compiler_params=pltpu.CompilerParams(vmem_limit_bytes=48 * 1024 * 1024),
        name="latent_qkv",
    )(latents, wq, wk, wv)


def latent_kernel(where_ref, q_ref, kv_ref, words_ref, wo_ref, out_ref):
    count, rows, _ = kv_ref.shape
    heads = []
    for head in range(2):
        cols = slice(head * head_dim, (head + 1) * head_dim)
        value_cols = slice(256 + head * head_dim, 256 + (head + 1) * head_dim)
        q = q_ref[:, cols]
        words = words_ref[head]

        def scores_of(t):
            s = nt_dot(q, kv_ref[t, :, cols])
            key = t * rows + lax.broadcasted_iota(jnp.int32, s.shape, 1)
            row = where_ref[0] * rows + lax.broadcasted_iota(jnp.int32, s.shape, 0)
            return jnp.where(key <= row, s, masked)

        summed, top, total = softmax_rows(
            scores_of,
            lambda t: (words & (1 << t)) != 0,
            lambda t: kv_ref[t, :, value_cols],
            count,
        )
        heads.append((summed * (keep_scale / total)).astype(bf16))
    attended = jnp.concatenate(heads, axis=1)
    for h in range(out_ref.shape[0]):
        out_ref[h] = jnp.dot(
            attended, wo_ref[:, h * 256 : (h + 1) * 256], preferred_element_type=f32
        ).astype(bf16)


def latent_attention(where, q, kv, words, wo, head_count):
    rows, columns = q.shape
    spec = pltpu.PrefetchScalarGridSpec(
        num_scalar_prefetch=1,
        grid=(1,),
        in_specs=[
            pl.BlockSpec(q.shape, lambda i, at: (0, 0)),
            pl.BlockSpec(kv.shape, lambda i, at: (0, 0, 0)),
            pl.BlockSpec((2, rows, 128), lambda i, at: (0, at[0], 0)),
            pl.BlockSpec(wo.shape, lambda i, at: (0, 0)),
        ],
        out_specs=pl.BlockSpec((head_count, rows, columns), lambda i, at: (0, 0, 0)),
    )
    return pl.pallas_call(
        latent_kernel,
        grid_spec=spec,
        out_shape=jax.ShapeDtypeStruct((head_count, rows, columns), bf16),
        compiler_params=params(),
        name="latent_attention",
    )(where, q, kv, words, wo)


def exchange(value, axis):
    return lax.all_to_all(value, axis, 0, 0, tiled=True)


def scatter_pairs(held, seq_index):
    count = held.shape[0]
    pair = held[count - 1]
    for k in range(count - 1):
        got = lax.ppermute(held[k], "seq", [(2 * count - 1, 2 * k + 1)])
        pair = jnp.where(seq_index == 2 * k + 1, got, pair)
    passed = lax.ppermute(pair[0], "seq", [(k + 1, k) for k in range(0, 2 * count, 2)])
    return jnp.where(seq_index % 2 == 0, passed, pair[1])


def per_device(
    context,
    wq_cross,
    wk_cross,
    wv_cross,
    wo_cross,
    wq_latent,
    wk_latent,
    wv_latent,
    wo_latent,
    cross_keep,
    latent_keep,
    residual_keep,
):
    seq_count = lax.axis_size("seq")
    head_count = lax.axis_size("head")
    root = seq_count - 1
    seq_index = lax.axis_index("seq").astype(jnp.int32)
    head_index = lax.axis_index("head").astype(jnp.int32)
    where = jnp.stack([seq_index, head_index])

    chunks = exchange(query_chunks(where, context, wq_cross, seq_count), "seq")
    keys, values = keys_values(context, wk_cross, wv_cross)
    own_queries, keys, values = lax.optimization_barrier((chunks[root], keys, values))
    queries = exchange(
        jnp.broadcast_to(own_queries[None], (seq_count, *own_queries.shape)), "seq"
    )
    rows, columns = own_queries.shape
    held = lax.dynamic_slice_in_dim(context, head_index * columns, columns, 1)
    held, _ = lax.optimization_barrier((held, own_queries))
    inputs = scatter_pairs(held.reshape(seq_count // 2, 2, rows, columns), seq_index)
    parts = cross_attention(where, queries, keys, values, cross_keep, root)
    parts = exchange(parts, "seq")
    branch = combine(parts, wo_cross, head_count)
    branch = exchange(branch, "head")
    latents = residual(where, branch, inputs, 0, residual_keep, 0)
    all_columns = lax.all_gather(latents, "head", axis=0, tiled=False)
    q, kv = latent_qkv(all_columns, wq_latent, wk_latent, wv_latent, seq_count)
    kv = exchange(kv, "seq")
    branch = latent_attention(where, q, kv, latent_keep, wo_latent, head_count)
    branch = exchange(branch, "head")
    return residual(where, branch, latents, 0, residual_keep, 1)


def solution(mesh):
    in_specs = (
        P("seq", None),
        P(None, "head"),
        P(None, "head"),
        P(None, "head"),
        P("head", None),
        P(None, "head"),
        P(None, "head"),
        P(None, "head"),
        P("head", None),
        P("head", None, "seq"),
        P("head", None, None),
        P(),
    )
    out_specs = P("seq", "head")
    return jax.shard_map(
        per_device, mesh=mesh, in_specs=in_specs, out_specs=out_specs, check_vma=False
    )
```

```python
import math

import jax
import jax.numpy as jnp
from jax import lax
from jax.experimental import pallas as pl
from jax.experimental.pallas import tpu as pltpu
from jax.sharding import PartitionSpec as P


bf16 = jnp.bfloat16
f32 = jnp.float32
keep_scale = 8.0 / 7.0
masked = -1e30
head_dim = 128
query_scale = math.log2(math.e) / math.sqrt(head_dim)
stat_rows = 16


def params(limit=48):
    return pltpu.CompilerParams(
        dimension_semantics=("arbitrary",), vmem_limit_bytes=limit * 1024 * 1024
    )


def row_scale(rows):
    wide = rows.astype(f32)
    mean_square = jnp.mean(wide * wide, axis=-1, keepdims=True)
    return lax.rsqrt(mean_square + 1e-06)


def query_kernel(root, where_ref, x_ref, w_ref, out_ref):
    @pl.when(where_ref[0] == root)
    def _():
        x = x_ref[...]
        product = jnp.dot(x, w_ref[...], preferred_element_type=f32)
        out_ref[...] = (
            (product * (row_scale(x) * query_scale)).astype(bf16).reshape(out_ref.shape)
        )


def query_chunks(where, context, wq, seq_count):
    tok_rows, width = context.shape
    columns = wq.shape[1]
    rows = tok_rows // seq_count
    group = 4
    root = seq_count - 1
    spec = pltpu.PrefetchScalarGridSpec(
        num_scalar_prefetch=1,
        grid=(seq_count // group,),
        in_specs=[
            pl.BlockSpec((rows * group, width), lambda i, at: (jnp.where(at[0] == root, i, 0), 0)),
            pl.BlockSpec((width, columns), lambda i, at: (0, 0)),
        ],
        out_specs=pl.BlockSpec((group, rows, columns), lambda i, at: (i, 0, 0)),
    )
    return pl.pallas_call(
        lambda *refs: query_kernel(root, *refs),
        grid_spec=spec,
        out_shape=jax.ShapeDtypeStruct((seq_count, rows, columns), bf16),
        compiler_params=params(52),
        name="queries",
    )(where, context, wq)


def kv_kernel(x_ref, wk_ref, wv_ref, k_ref, v_ref):
    x = x_ref[...]
    scale = row_scale(x)
    k_ref[...] = (jnp.dot(x, wk_ref[...], preferred_element_type=f32) * scale).astype(bf16)
    v_ref[...] = (jnp.dot(x, wv_ref[...], preferred_element_type=f32) * scale).astype(bf16)


def keys_values(context, wk, wv):
    tok_rows, width = context.shape
    columns = wk.shape[1]
    block = 512
    return pl.pallas_call(
        kv_kernel,
        grid=(tok_rows // block,),
        in_specs=[
            pl.BlockSpec((block, width), lambda i: (i, 0)),
            pl.BlockSpec((width, columns), lambda i: (0, 0)),
            pl.BlockSpec((width, columns), lambda i: (0, 0)),
        ],
        out_specs=[pl.BlockSpec((block, columns), lambda i: (i, 0))] * 2,
        out_shape=[jax.ShapeDtypeStruct((tok_rows, columns), bf16)] * 2,
        compiler_params=params(52),
        name="keys_values",
    )(context, wk, wv)


def softmax_rows(scores_of, keep_of, values_of, pieces):
    scores = [scores_of(b) for b in range(pieces)]
    top = scores[0]
    for s in scores[1:]:
        top = jnp.maximum(top, s)
    top = jnp.max(top, axis=-1, keepdims=True)
    total = None
    summed = None
    for b in range(pieces):
        p = jnp.exp2(scores[b] - top)
        total = p if total is None else total + p
        kept = jnp.where(keep_of(b), p, 0.0).astype(bf16)
        part = jnp.dot(kept, values_of(b), preferred_element_type=f32)
        summed = part if summed is None else summed + part
    total = jnp.sum(total, axis=-1, keepdims=True)
    return summed, top, total


def nt_dot(a, b):
    return lax.dot_general(a, b, (((1,), (1,)), ((), ())), preferred_element_type=f32)


def cross_kernel(root, n, where_ref, q_ref, k_ref, v_ref, words_ref, out_ref, s0_ref, s1_ref, m_ref):
    rows = n * head_dim
    wide = words_ref.shape[2]
    step = pl.program_id(0)
    following = jnp.minimum(step + 1, pl.num_programs(0) - 1)

    def run(causal):
        def score(head, block, b):
            cols = slice(head * head_dim, (head + 1) * head_dim)
            q = q_ref[pl.ds(block * n, n), :, cols].reshape(rows, head_dim)
            s = nt_dot(q, k_ref[b * wide : (b + 1) * wide, cols])
            if causal:
                key = b * wide + lax.broadcasted_iota(jnp.int32, s.shape, 1)
                row = block * rows + lax.broadcasted_iota(jnp.int32, s.shape, 0)
                s = jnp.where(key <= row, s, masked)
            return s

        def stage(head, next_block):
            ready, filling = (s0_ref, s1_ref) if head == 0 else (s1_ref, s0_ref)
            cols = slice(head * head_dim, (head + 1) * head_dim)
            words = words_ref[head].astype(jnp.int16)
            top = jnp.max(m_ref[head], axis=-1, keepdims=True)
            total = None
            summed = None
            next_top = None
            for b in range(8):
                s = score(1 - head, next_block, b)
                p = jnp.exp2(ready[b] - top)
                total = p if total is None else total + p
                kept = jnp.where((words & jnp.int16(1 << b)) != jnp.int16(0), p.astype(bf16), bf16(0))
                part = jnp.dot(
                    kept, v_ref[b * wide : (b + 1) * wide, cols], preferred_element_type=f32
                )
                summed = part if summed is None else summed + part
                filling[b] = s
                next_top = s if next_top is None else jnp.maximum(next_top, s)
            m_ref[1 - head] = next_top
            total = jnp.sum(total, axis=-1, keepdims=True)
            out = (summed * (keep_scale / total)).astype(bf16)
            for i in range(n):
                out_ref[i, head * head_dim : (head + 1) * head_dim, :] = out[
                    i * head_dim : (i + 1) * head_dim
                ]
            return top + jnp.log2(total)

        @pl.when(step == 0)
        def _():
            first_top = None
            for b in range(8):
                s = score(0, 0, b)
                s0_ref[b] = s
                first_top = s if first_top is None else jnp.maximum(first_top, s)
            m_ref[0] = first_top

        sums = [stage(0, step), stage(1, following)]
        lanes = lax.broadcasted_iota(jnp.int32, (rows, head_dim), 1)
        stats = jnp.zeros((rows, head_dim), f32)
        for head, lse in enumerate(sums):
            high = lse.astype(bf16).astype(f32)
            middle = (lse - high).astype(bf16).astype(f32)
            low = lse - high - middle
            for j, piece in enumerate((high, middle, low)):
                stats = jnp.where(lanes == head * 3 + j, piece, stats)
        for i in range(n):
            out_ref[i, 2 * head_dim :, :] = (
                stats[i * head_dim : (i + 1) * head_dim].T[:stat_rows].astype(bf16)
            )

    @pl.when(where_ref[0] == root)
    def _():
        run(True)

    @pl.when(where_ref[0] != root)
    def _():
        run(False)


def cross_attention(where, queries, keys, values, words, root):
    count = queries.shape[0]
    n = 4
    rows = n * head_dim
    wide = words.shape[2]
    whole = pl.Buffered(1)
    spec = pltpu.PrefetchScalarGridSpec(
        num_scalar_prefetch=1,
        grid=(count // n,),
        in_specs=[
            pl.BlockSpec(queries.shape, lambda i, at: (0, 0, 0), pipeline_mode=whole),
            pl.BlockSpec(keys.shape, lambda i, at: (0, 0), pipeline_mode=whole),
            pl.BlockSpec(values.shape, lambda i, at: (0, 0), pipeline_mode=whole),
            pl.BlockSpec((2, rows, wide), lambda i, at: (0, i, 0)),
        ],
        out_specs=pl.BlockSpec((n, 2 * head_dim + stat_rows, head_dim), lambda i, at: (i, 0, 0)),
        scratch_shapes=[
            pltpu.VMEM((8, rows, wide), f32),
            pltpu.VMEM((8, rows, wide), f32),
            pltpu.VMEM((2, rows, wide), f32),
        ],
    )
    return pl.pallas_call(
        lambda *refs: cross_kernel(root, n, *refs),
        grid_spec=spec,
        out_shape=jax.ShapeDtypeStruct((count, 2 * head_dim + stat_rows, head_dim), bf16),
        compiler_params=params(52),
        name="cross_attention",
    )(where, queries, keys, values, words)


def project_shares(attended, wo_of, core, own_ref, theirs_ref):
    for h in range(2 * own_ref.shape[0]):
        share = jnp.dot(attended, wo_of(h), preferred_element_type=f32)

        @pl.when(core == h % 2)
        def _():
            own_ref[h // 2] = share

        @pl.when(core != h % 2)
        def _():
            theirs_ref[h // 2] = share.astype(bf16)


def share_shapes(pairs, rows, columns):
    return [
        jax.ShapeDtypeStruct((pairs, rows, columns), f32),
        jax.ShapeDtypeStruct((pairs, rows, columns), bf16),
    ]


def combine_kernel(where_ref, parts_ref, wo_hbm, own_ref, theirs_ref, wo_ref, sem):
    fetch = pltpu.make_async_copy(wo_hbm, wo_ref, sem)
    fetch.start()
    count = parts_ref.shape[0]
    rows = head_dim
    heads = []
    stats = parts_ref[:, 2 * rows :, :].astype(f32)
    for head in range(2):
        lse = stats[:, head * 3] + stats[:, head * 3 + 1] + stats[:, head * 3 + 2]
        weight = jnp.exp2(lse - jnp.max(lse, axis=0, keepdims=True))
        weight = weight / jnp.sum(weight, axis=0, keepdims=True)
        weight = jnp.concatenate([weight, jnp.zeros((rows - count, rows), f32)], axis=0).T
        mixed = None
        for s in range(count):
            part = parts_ref[s, head * rows : (head + 1) * rows, :].astype(f32)
            part = part * weight[:, s : s + 1]
            mixed = part if mixed is None else mixed + part
        heads.append(mixed.astype(bf16))
    attended = jnp.concatenate(heads, axis=1)
    fetch.wait()
    project_shares(
        attended, lambda h: wo_ref[:, h * 256 : (h + 1) * 256], where_ref[1] % 2, own_ref, theirs_ref
    )


def combine(where, parts, wo, pairs):
    whole = lambda i, at: (0, 0, 0)
    spec = pltpu.PrefetchScalarGridSpec(
        num_scalar_prefetch=1,
        grid=(1,),
        in_specs=[pl.BlockSpec(parts.shape, whole), pl.BlockSpec(memory_space=pl.ANY)],
        out_specs=[pl.BlockSpec((pairs, head_dim, 256), whole)] * 2,
        scratch_shapes=[pltpu.VMEM(wo.shape, bf16), pltpu.SemaphoreType.DMA(())],
    )
    return pl.pallas_call(
        combine_kernel,
        grid_spec=spec,
        out_shape=share_shapes(pairs, head_dim, 256),
        compiler_params=params(),
        name="combine",
    )(where, parts, wo)


def chip_sum_kernel(where_ref, own_ref, got_ref, kept_ref, *out_refs):
    pairs = own_ref.shape[0]
    place = where_ref[1] // 2
    kept_ref[...] = own_ref[place] + got_ref[place].astype(f32)
    for d, out_ref in enumerate(out_refs, 1):
        target = lax.rem(place + d, pairs)
        out_ref[...] = (own_ref[target] + got_ref[target].astype(f32)).astype(bf16)


def chip_sum(where, own, got):
    pairs, rows, columns = own.shape
    flat = lambda i, at: (0, 0)
    spec = pltpu.PrefetchScalarGridSpec(
        num_scalar_prefetch=1,
        grid=(1,),
        in_specs=[pl.BlockSpec(own.shape, lambda i, at: (0, 0, 0))] * 2,
        out_specs=[pl.BlockSpec((rows, columns), flat)] * pairs,
    )
    return pl.pallas_call(
        chip_sum_kernel,
        grid_spec=spec,
        out_shape=[jax.ShapeDtypeStruct((rows, columns), f32)]
        + [jax.ShapeDtypeStruct((rows, columns), bf16)] * (pairs - 1),
        compiler_params=params(),
        name="chip_sum",
    )(where, own, got)


def residual_kernel(where_ref, *refs):
    *share_refs, base_ref, words_ref, out_ref = refs
    total = share_refs[0][...].astype(f32)
    for ref in share_refs[1:]:
        total = total + ref[...].astype(f32)
    words = words_ref[0]
    for half in range(2):
        cols = slice(half * 128, half * 128 + 128)
        flag = (jnp.right_shift(words, where_ref[1] * 2 + half) & 1).astype(f32)
        base = base_ref[:, cols].astype(f32)
        out_ref[:, cols] = (base + flag * keep_scale * total[:, cols]).astype(bf16)


def residual(where, shares, base, words, index):
    rows, columns = base.shape
    flat = lambda i, at: (0, 0)
    spec = pltpu.PrefetchScalarGridSpec(
        num_scalar_prefetch=1,
        grid=(1,),
        in_specs=[pl.BlockSpec((rows, columns), flat)] * (len(shares) + 1)
        + [pl.BlockSpec((1, rows, 128), lambda i, at: (index, at[0], 0))],
        out_specs=pl.BlockSpec((rows, columns), flat),
    )
    return pl.pallas_call(
        residual_kernel,
        grid_spec=spec,
        out_shape=jax.ShapeDtypeStruct((rows, columns), bf16),
        compiler_params=params(),
        name="residual",
    )(where, *shares, base, words)


def latent_qkv_kernel(where_ref, near_ref, far_ref, wq_ref, wk_ref, wv_ref, q_ref, kv_ref):
    pairs, rows, columns = near_ref.shape
    place = where_ref[1] // 2
    core = where_ref[1] % 2
    pieces = []
    for d in range(pairs):
        chip = lax.rem(place + pairs - d, pairs)
        for ref, side in ((near_ref, core), (far_ref, 1 - core)):
            first = pl.multiple_of((2 * chip + side) * columns, columns)
            pieces.append((ref[d], first))
    squares = None
    for piece, _ in pieces:
        wide = piece.astype(f32)
        part = jnp.sum(wide * wide, axis=-1, keepdims=True)
        squares = part if squares is None else squares + part
    scale = lax.rsqrt(squares / (2 * pairs * columns) + 1e-06)

    def project(w_ref):
        total = None
        for piece, first in pieces:
            part = jnp.dot(piece, w_ref[pl.ds(first, columns), :], preferred_element_type=f32)
            total = part if total is None else total + part
        return total * scale

    q_ref[...] = (project(wq_ref) * query_scale).astype(bf16)
    keys = project(wk_ref).astype(bf16)
    values = project(wv_ref).astype(bf16)
    for s in range(kv_ref.shape[0]):
        kv_ref[s, :, :columns] = keys
        kv_ref[s, :, columns:] = values


def latent_qkv(where, near, far, wq, wk, wv, seq_count):
    pairs, rows, columns = near.shape
    spec = pltpu.PrefetchScalarGridSpec(
        num_scalar_prefetch=1,
        grid=(1,),
        in_specs=[pl.BlockSpec(near.shape, lambda i, at: (0, 0, 0))] * 2
        + [pl.BlockSpec(wq.shape, lambda i, at: (0, 0))] * 3,
        out_specs=[
            pl.BlockSpec((rows, columns), lambda i, at: (0, 0)),
            pl.BlockSpec((seq_count, rows, 2 * columns), lambda i, at: (0, 0, 0)),
        ],
    )
    return pl.pallas_call(
        latent_qkv_kernel,
        grid_spec=spec,
        out_shape=[
            jax.ShapeDtypeStruct((rows, columns), bf16),
            jax.ShapeDtypeStruct((seq_count, rows, 2 * columns), bf16),
        ],
        compiler_params=params(),
        name="latent_qkv",
    )(where, near, far, wq, wk, wv)


def latent_kernel(where_ref, q_ref, kv_ref, words_ref, wo_ref, own_ref, theirs_ref):
    count, rows, _ = kv_ref.shape
    heads = []
    for head in range(2):
        cols = slice(head * head_dim, (head + 1) * head_dim)
        value_cols = slice(256 + head * head_dim, 256 + (head + 1) * head_dim)
        q = q_ref[:, cols]
        words = words_ref[head]

        def scores_of(t):
            s = nt_dot(q, kv_ref[t, :, cols])
            key = t * rows + lax.broadcasted_iota(jnp.int32, s.shape, 1)
            row = where_ref[0] * rows + lax.broadcasted_iota(jnp.int32, s.shape, 0)
            return jnp.where(key <= row, s, masked)

        summed, top, total = softmax_rows(
            scores_of,
            lambda t: (words & (1 << t)) != 0,
            lambda t: kv_ref[t, :, value_cols],
            count,
        )
        heads.append((summed * (keep_scale / total)).astype(bf16))
    attended = jnp.concatenate(heads, axis=1)
    project_shares(
        attended, lambda h: wo_ref[:, h * 256 : (h + 1) * 256], where_ref[1] % 2, own_ref, theirs_ref
    )


def latent_attention(where, q, kv, words, wo, pairs):
    rows, columns = q.shape
    spec = pltpu.PrefetchScalarGridSpec(
        num_scalar_prefetch=1,
        grid=(1,),
        in_specs=[
            pl.BlockSpec(q.shape, lambda i, at: (0, 0)),
            pl.BlockSpec(kv.shape, lambda i, at: (0, 0, 0)),
            pl.BlockSpec((2, rows, 128), lambda i, at: (0, at[0], 0)),
            pl.BlockSpec(wo.shape, lambda i, at: (0, 0)),
        ],
        out_specs=[pl.BlockSpec((pairs, rows, columns), lambda i, at: (0, 0, 0))] * 2,
    )
    return pl.pallas_call(
        latent_kernel,
        grid_spec=spec,
        out_shape=share_shapes(pairs, rows, columns),
        compiler_params=params(),
        name="latent_attention",
    )(where, q, kv, words, wo)


def exchange(value, axis):
    return lax.all_to_all(value, axis, 0, 0, tiled=True)


def to_partner(value):
    count = lax.axis_size("head")
    return lax.ppermute(value, "head", [(i, i ^ 1) for i in range(count)])


def along_chips(value, distance):
    count = lax.axis_size("head")
    return lax.ppermute(
        value, "head", [(i, (i + 2 * distance) % count) for i in range(count)]
    )


def head_sum(where, own, theirs):
    kept, *sent = chip_sum(where, own, to_partner(theirs))
    return [kept] + [along_chips(value, d) for d, value in enumerate(sent, 1)]


def scatter_pairs(held, seq_index):
    count = held.shape[0]
    pair = held[count - 1]
    for k in range(count - 1):
        got = lax.ppermute(held[k], "seq", [(2 * count - 1, 2 * k + 1)])
        pair = jnp.where(seq_index == 2 * k + 1, got, pair)
    passed = lax.ppermute(pair[0], "seq", [(k + 1, k) for k in range(0, 2 * count, 2)])
    return jnp.where(seq_index % 2 == 0, passed, pair[1])


def per_device(
    context,
    wq_cross,
    wk_cross,
    wv_cross,
    wo_cross,
    wq_latent,
    wk_latent,
    wv_latent,
    wo_latent,
    cross_keep,
    latent_keep,
    residual_keep,
):
    seq_count = lax.axis_size("seq")
    head_count = lax.axis_size("head")
    root = seq_count - 1
    seq_index = lax.axis_index("seq").astype(jnp.int32)
    head_index = lax.axis_index("head").astype(jnp.int32)
    where = jnp.stack([seq_index, head_index])

    chunks = exchange(query_chunks(where, context, wq_cross, seq_count), "seq")
    keys, values = keys_values(context, wk_cross, wv_cross)
    own_queries, keys, values = lax.optimization_barrier((chunks[root], keys, values))
    queries = exchange(
        jnp.broadcast_to(own_queries[None], (seq_count, *own_queries.shape)), "seq"
    )
    rows, columns = own_queries.shape
    held = lax.dynamic_slice_in_dim(context, head_index * columns, columns, 1)
    held, _ = lax.optimization_barrier((held, own_queries))
    inputs = scatter_pairs(held.reshape(seq_count // 2, 2, rows, columns), seq_index)
    queries, inputs = lax.optimization_barrier((queries, inputs))
    parts = cross_attention(where, queries, keys, values, cross_keep, root)
    parts = exchange(parts, "seq")
    pairs = head_count // 2
    own, theirs = combine(where, parts, wo_cross, pairs)
    latents = residual(where, head_sum(where, own, theirs), inputs, residual_keep, 0)
    near = jnp.stack([latents] + [along_chips(latents, d) for d in range(1, pairs)])
    far = to_partner(near)
    q, kv = latent_qkv(where, near, far, wq_latent, wk_latent, wv_latent, seq_count)
    kv = exchange(kv, "seq")
    own, theirs = latent_attention(where, q, kv, latent_keep, wo_latent, pairs)
    return residual(where, head_sum(where, own, theirs), latents, residual_keep, 1)


def solution(mesh):
    in_specs = (
        P("seq", None),
        P(None, "head"),
        P(None, "head"),
        P(None, "head"),
        P("head", None),
        P(None, "head"),
        P(None, "head"),
        P(None, "head"),
        P("head", None),
        P("head", None, "seq"),
        P("head", None, None),
        P(),
    )
    out_specs = P("seq", "head")
    return jax.shard_map(
        per_device, mesh=mesh, in_specs=in_specs, out_specs=out_specs, check_vma=False
    )
```

```python
import math

import jax
import jax.numpy as jnp
from jax import lax
from jax.experimental import pallas as pl
from jax.experimental.pallas import tpu as pltpu
from jax.sharding import PartitionSpec as P


bf16 = jnp.bfloat16
f32 = jnp.float32
keep_scale = 8.0 / 7.0
masked = -1e30
head_dim = 128
query_scale = math.log2(math.e) / math.sqrt(head_dim)
stat_rows = 16


def params(limit=48):
    return pltpu.CompilerParams(
        dimension_semantics=("arbitrary",), vmem_limit_bytes=limit * 1024 * 1024
    )


def row_scale(rows):
    wide = rows.astype(f32)
    mean_square = jnp.mean(wide * wide, axis=-1, keepdims=True)
    return lax.rsqrt(mean_square + 1e-06)


def query_kernel(root, where_ref, x_ref, w_ref, out_ref):
    @pl.when(where_ref[0] == root)
    def _():
        x = x_ref[...]
        product = jnp.dot(x, w_ref[...], preferred_element_type=f32)
        out_ref[...] = (
            (product * (row_scale(x) * query_scale)).astype(bf16).reshape(out_ref.shape)
        )


def query_chunks(where, context, wq, seq_count):
    tok_rows, width = context.shape
    columns = wq.shape[1]
    rows = tok_rows // seq_count
    group = 4
    root = seq_count - 1
    spec = pltpu.PrefetchScalarGridSpec(
        num_scalar_prefetch=1,
        grid=(seq_count // group,),
        in_specs=[
            pl.BlockSpec((rows * group, width), lambda i, at: (jnp.where(at[0] == root, i, 0), 0)),
            pl.BlockSpec((width, columns), lambda i, at: (0, 0)),
        ],
        out_specs=pl.BlockSpec((group, rows, columns), lambda i, at: (i, 0, 0)),
    )
    return pl.pallas_call(
        lambda *refs: query_kernel(root, *refs),
        grid_spec=spec,
        out_shape=jax.ShapeDtypeStruct((seq_count, rows, columns), bf16),
        compiler_params=params(52),
        name="queries",
    )(where, context, wq)


def kv_kernel(x_ref, wk_ref, wv_ref, k_ref, v_ref):
    x = x_ref[...]
    scale = row_scale(x)
    k_ref[...] = (jnp.dot(x, wk_ref[...], preferred_element_type=f32) * scale).astype(bf16)
    v_ref[...] = (jnp.dot(x, wv_ref[...], preferred_element_type=f32) * scale).astype(bf16)


def keys_values(context, wk, wv):
    tok_rows, width = context.shape
    columns = wk.shape[1]
    block = 512
    return pl.pallas_call(
        kv_kernel,
        grid=(tok_rows // block,),
        in_specs=[
            pl.BlockSpec((block, width), lambda i: (i, 0)),
            pl.BlockSpec((width, columns), lambda i: (0, 0)),
            pl.BlockSpec((width, columns), lambda i: (0, 0)),
        ],
        out_specs=[pl.BlockSpec((block, columns), lambda i: (i, 0))] * 2,
        out_shape=[jax.ShapeDtypeStruct((tok_rows, columns), bf16)] * 2,
        compiler_params=params(52),
        name="keys_values",
    )(context, wk, wv)


def softmax_rows(scores_of, keep_of, values_of, pieces):
    scores = [scores_of(b) for b in range(pieces)]
    top = scores[0]
    for s in scores[1:]:
        top = jnp.maximum(top, s)
    top = jnp.max(top, axis=-1, keepdims=True)
    total = None
    summed = None
    for b in range(pieces):
        p = jnp.exp2(scores[b] - top)
        total = p if total is None else total + p
        kept = jnp.where(keep_of(b), p, 0.0).astype(bf16)
        part = jnp.dot(kept, values_of(b), preferred_element_type=f32)
        summed = part if summed is None else summed + part
    total = jnp.sum(total, axis=-1, keepdims=True)
    return summed, top, total


def nt_dot(a, b):
    return lax.dot_general(a, b, (((1,), (1,)), ((), ())), preferred_element_type=f32)


def cross_kernel(
    root, n, steps, where_ref, q_ref, k_ref, v_ref, words_ref, out_ref, s0_ref, s1_ref, m_ref
):
    rows = n * head_dim
    wide = words_ref.shape[2]
    step = pl.program_id(0)
    following = jnp.minimum(step + 1, steps - 1)

    def score(head, block, b, causal):
        cols = slice(head * head_dim, (head + 1) * head_dim)
        q = q_ref[pl.ds(block * n, n), :, cols].reshape(rows, head_dim)
        s = nt_dot(q, k_ref[b * wide : (b + 1) * wide, cols])
        if causal and (b + 1) * wide > block * rows:
            key = b * wide + lax.broadcasted_iota(jnp.int32, s.shape, 1)
            row = block * rows + lax.broadcasted_iota(jnp.int32, s.shape, 0)
            s = jnp.where(key <= row, s, masked)
        return s

    def stage(head, next_block, pieces, next_pieces, causal):
        ready, filling = (s0_ref, s1_ref) if head == 0 else (s1_ref, s0_ref)
        cols = slice(head * head_dim, (head + 1) * head_dim)
        words = words_ref[head].astype(jnp.int16)
        top = jnp.max(m_ref[head], axis=-1, keepdims=True)
        total = None
        summed = None
        next_top = None
        for b in range(max(pieces, next_pieces)):
            if b < next_pieces:
                s = score(1 - head, next_block, b, causal)
            if b < pieces:
                p = jnp.exp2(ready[b] - top)
                total = p if total is None else total + p
                kept = jnp.where(
                    (words & jnp.int16(1 << b)) != jnp.int16(0), p.astype(bf16), bf16(0)
                )
                part = jnp.dot(
                    kept, v_ref[b * wide : (b + 1) * wide, cols], preferred_element_type=f32
                )
                summed = part if summed is None else summed + part
            if b < next_pieces:
                filling[b] = s
                next_top = s if next_top is None else jnp.maximum(next_top, s)
        if next_pieces:
            m_ref[1 - head] = next_top
        total = jnp.sum(total, axis=-1, keepdims=True)
        out = (summed * (keep_scale / total)).astype(bf16)
        for i in range(n):
            out_ref[i, head * head_dim : (head + 1) * head_dim, :] = out[
                i * head_dim : (i + 1) * head_dim
            ]
        return top + jnp.log2(total)

    def first_scores(pieces, causal):
        first_top = None
        for b in range(pieces):
            s = score(0, 0, b, causal)
            s0_ref[b] = s
            first_top = s if first_top is None else jnp.maximum(first_top, s)
        m_ref[0] = first_top

    def run(block, next_block, pieces, next_pieces, causal):
        sums = [
            stage(0, block, pieces, pieces, causal),
            stage(1, next_block, pieces, next_pieces, causal),
        ]
        lanes = lax.broadcasted_iota(jnp.int32, (rows, head_dim), 1)
        stats = jnp.zeros((rows, head_dim), f32)
        for head, lse in enumerate(sums):
            high = lse.astype(bf16).astype(f32)
            middle = (lse - high).astype(bf16).astype(f32)
            low = lse - high - middle
            for j, piece in enumerate((high, middle, low)):
                stats = jnp.where(lanes == head * 3 + j, piece, stats)
        for i in range(n):
            out_ref[i, 2 * head_dim :, :] = (
                stats[i * head_dim : (i + 1) * head_dim].T[:stat_rows].astype(bf16)
            )

    for k in range(steps):

        @pl.when((where_ref[0] == root) & (step == k))
        def _():
            reach = [(j + 1) * rows // wide for j in range(steps)] + [0]
            if k == 0:
                first_scores(reach[0], True)
            run(k, k + 1, reach[k], reach[k + 1], True)

    @pl.when(where_ref[0] != root)
    def _():
        @pl.when(step == 0)
        def _():
            first_scores(8, False)

        run(step, following, 8, 8, False)


def cross_attention(where, queries, keys, values, words, root):
    count = queries.shape[0]
    n = 4
    rows = n * head_dim
    wide = words.shape[2]
    whole = pl.Buffered(1)
    spec = pltpu.PrefetchScalarGridSpec(
        num_scalar_prefetch=1,
        grid=(count // n,),
        in_specs=[
            pl.BlockSpec(queries.shape, lambda i, at: (0, 0, 0), pipeline_mode=whole),
            pl.BlockSpec(keys.shape, lambda i, at: (0, 0), pipeline_mode=whole),
            pl.BlockSpec(values.shape, lambda i, at: (0, 0), pipeline_mode=whole),
            pl.BlockSpec((2, rows, wide), lambda i, at: (0, i, 0)),
        ],
        out_specs=pl.BlockSpec((n, 2 * head_dim + stat_rows, head_dim), lambda i, at: (i, 0, 0)),
        scratch_shapes=[
            pltpu.VMEM((8, rows, wide), f32),
            pltpu.VMEM((8, rows, wide), f32),
            pltpu.VMEM((2, rows, wide), f32),
        ],
    )
    return pl.pallas_call(
        lambda *refs: cross_kernel(root, n, count // n, *refs),
        grid_spec=spec,
        out_shape=jax.ShapeDtypeStruct((count, 2 * head_dim + stat_rows, head_dim), bf16),
        compiler_params=params(52),
        cost_estimate=pl.CostEstimate(
            flops=8 * count * head_dim * keys.shape[0] * head_dim,
            transcendentals=2 * count * head_dim * keys.shape[0],
            bytes_accessed=4 * words.size,
        ),
        name="cross_attention",
    )(where, queries, keys, values, words)


def project_shares(attended, wo_ref, core, own_ref, theirs_ref):
    columns = own_ref.shape[2]
    for p in range(own_ref.shape[0]):
        for side, out_ref in ((core, own_ref), (1 - core, theirs_ref)):
            first = pl.multiple_of((2 * p + side) * columns, columns)
            share = jnp.dot(
                attended, wo_ref[:, pl.ds(first, columns)], preferred_element_type=f32
            )
            out_ref[p] = share.astype(out_ref.dtype)


def share_shapes(pairs, rows, columns):
    return [
        jax.ShapeDtypeStruct((pairs, rows, columns), f32),
        jax.ShapeDtypeStruct((pairs, rows, columns), bf16),
    ]


def combine_kernel(where_ref, parts_ref, wo_ref, own_ref, theirs_ref):
    count = parts_ref.shape[0]
    rows = head_dim
    heads = []
    stats = parts_ref[:, 2 * rows :, :].astype(f32)
    for head in range(2):
        lse = stats[:, head * 3] + stats[:, head * 3 + 1] + stats[:, head * 3 + 2]
        weight = jnp.exp2(lse - jnp.max(lse, axis=0, keepdims=True))
        weight = weight / jnp.sum(weight, axis=0, keepdims=True)
        weight = jnp.concatenate([weight, jnp.zeros((rows - count, rows), f32)], axis=0).T
        mixed = None
        for s in range(count):
            part = parts_ref[s, head * rows : (head + 1) * rows, :].astype(f32)
            part = part * weight[:, s : s + 1]
            mixed = part if mixed is None else mixed + part
        heads.append(mixed.astype(bf16))
    attended = jnp.concatenate(heads, axis=1)
    project_shares(attended, wo_ref, where_ref[1] % 2, own_ref, theirs_ref)


def combine(where, parts, wo, pairs):
    whole = lambda i, at: (0, 0, 0)
    spec = pltpu.PrefetchScalarGridSpec(
        num_scalar_prefetch=1,
        grid=(1,),
        in_specs=[
            pl.BlockSpec(parts.shape, whole),
            pl.BlockSpec(wo.shape, lambda i, at: (0, 0)),
        ],
        out_specs=[pl.BlockSpec((pairs, head_dim, 256), whole)] * 2,
    )
    return pl.pallas_call(
        combine_kernel,
        grid_spec=spec,
        out_shape=share_shapes(pairs, head_dim, 256),
        compiler_params=params(16),
        name="combine",
    )(where, parts, wo)


def chip_sum_kernel(where_ref, own_ref, got_ref, kept_ref, *out_refs):
    pairs = own_ref.shape[0]
    place = where_ref[1] // 2
    kept_ref[...] = own_ref[place] + got_ref[place].astype(f32)
    for d, out_ref in enumerate(out_refs, 1):
        target = lax.rem(place + d, pairs)
        out_ref[...] = (own_ref[target] + got_ref[target].astype(f32)).astype(bf16)


def chip_sum(where, own, got):
    pairs, rows, columns = own.shape
    flat = lambda i, at: (0, 0)
    spec = pltpu.PrefetchScalarGridSpec(
        num_scalar_prefetch=1,
        grid=(1,),
        in_specs=[pl.BlockSpec(own.shape, lambda i, at: (0, 0, 0))] * 2,
        out_specs=[pl.BlockSpec((rows, columns), flat)] * pairs,
    )
    return pl.pallas_call(
        chip_sum_kernel,
        grid_spec=spec,
        out_shape=[jax.ShapeDtypeStruct((rows, columns), f32)]
        + [jax.ShapeDtypeStruct((rows, columns), bf16)] * (pairs - 1),
        compiler_params=params(8),
        name="chip_sum",
    )(where, own, got)


def residual_kernel(where_ref, *refs):
    *share_refs, base_ref, words_ref, out_ref = refs
    total = share_refs[0][...].astype(f32)
    for ref in share_refs[1:]:
        total = total + ref[...].astype(f32)
    words = words_ref[0]
    for half in range(2):
        cols = slice(half * 128, half * 128 + 128)
        flag = (jnp.right_shift(words, where_ref[1] * 2 + half) & 1).astype(f32)
        base = base_ref[:, cols].astype(f32)
        out_ref[:, cols] = (base + flag * keep_scale * total[:, cols]).astype(bf16)


def residual(where, shares, base, words, index):
    rows, columns = base.shape
    flat = lambda i, at: (0, 0)
    spec = pltpu.PrefetchScalarGridSpec(
        num_scalar_prefetch=1,
        grid=(1,),
        in_specs=[pl.BlockSpec((rows, columns), flat)] * (len(shares) + 1)
        + [pl.BlockSpec((1, rows, 128), lambda i, at: (index, at[0], 0))],
        out_specs=pl.BlockSpec((rows, columns), flat),
    )
    return pl.pallas_call(
        residual_kernel,
        grid_spec=spec,
        out_shape=jax.ShapeDtypeStruct((rows, columns), bf16),
        compiler_params=params(8),
        name="residual",
    )(where, *shares, base, words)


def latent_qkv_kernel(where_ref, near_ref, far_ref, wq_ref, wk_ref, wv_ref, q_ref, kv_ref):
    pairs, _, columns = near_ref.shape
    place = where_ref[1] // 2
    core = where_ref[1] % 2
    pieces = []
    for d in range(pairs):
        chip = lax.rem(place + pairs - d, pairs)
        for ref, side in ((near_ref, core), (far_ref, 1 - core)):
            first = pl.multiple_of((2 * chip + side) * columns, columns)
            pieces.append((ref[d], first))
    squares = None
    for piece, _ in pieces:
        wide = piece.astype(f32)
        part = jnp.sum(wide * wide, axis=-1, keepdims=True)
        squares = part if squares is None else squares + part
    scale = lax.rsqrt(squares / (2 * pairs * columns) + 1e-06)

    def project(w_ref):
        total = None
        for piece, first in pieces:
            part = jnp.dot(piece, w_ref[pl.ds(first, columns), :], preferred_element_type=f32)
            total = part if total is None else total + part
        return total * scale

    q_ref[...] = (project(wq_ref) * query_scale).astype(bf16)
    keys = project(wk_ref).astype(bf16)
    values = project(wv_ref).astype(bf16)
    for s in range(kv_ref.shape[0]):
        kv_ref[s, :, :columns] = keys
        kv_ref[s, :, columns:] = values


def latent_qkv(where, near, far, wq, wk, wv, seq_count):
    _, rows, columns = near.shape
    spec = pltpu.PrefetchScalarGridSpec(
        num_scalar_prefetch=1,
        grid=(1,),
        in_specs=[pl.BlockSpec(near.shape, lambda i, at: (0, 0, 0))] * 2
        + [pl.BlockSpec(wq.shape, lambda i, at: (0, 0))] * 3,
        out_specs=[
            pl.BlockSpec((rows, columns), lambda i, at: (0, 0)),
            pl.BlockSpec((seq_count, rows, 2 * columns), lambda i, at: (0, 0, 0)),
        ],
    )
    return pl.pallas_call(
        latent_qkv_kernel,
        grid_spec=spec,
        out_shape=[
            jax.ShapeDtypeStruct((rows, columns), bf16),
            jax.ShapeDtypeStruct((seq_count, rows, 2 * columns), bf16),
        ],
        compiler_params=params(24),
        name="latent_qkv",
    )(where, near, far, wq, wk, wv)


def latent_kernel(where_ref, q_ref, kv_ref, words_ref, wo_ref, own_ref, theirs_ref):
    count, rows, _ = kv_ref.shape
    heads = []
    for head in range(2):
        cols = slice(head * head_dim, (head + 1) * head_dim)
        value_cols = slice(256 + head * head_dim, 256 + (head + 1) * head_dim)
        q = q_ref[:, cols]
        words = words_ref[head]

        def scores_of(t):
            s = nt_dot(q, kv_ref[t, :, cols])
            key = t * rows + lax.broadcasted_iota(jnp.int32, s.shape, 1)
            row = where_ref[0] * rows + lax.broadcasted_iota(jnp.int32, s.shape, 0)
            return jnp.where(key <= row, s, masked)

        summed, _, total = softmax_rows(
            scores_of,
            lambda t: (words & (1 << t)) != 0,
            lambda t: kv_ref[t, :, value_cols],
            count,
        )
        heads.append((summed * (keep_scale / total)).astype(bf16))
    attended = jnp.concatenate(heads, axis=1)
    project_shares(attended, wo_ref, where_ref[1] % 2, own_ref, theirs_ref)


def latent_attention(where, q, kv, words, wo, pairs):
    rows, columns = q.shape
    spec = pltpu.PrefetchScalarGridSpec(
        num_scalar_prefetch=1,
        grid=(1,),
        in_specs=[
            pl.BlockSpec(q.shape, lambda i, at: (0, 0)),
            pl.BlockSpec(kv.shape, lambda i, at: (0, 0, 0)),
            pl.BlockSpec((2, rows, 128), lambda i, at: (0, at[0], 0)),
            pl.BlockSpec(wo.shape, lambda i, at: (0, 0)),
        ],
        out_specs=[pl.BlockSpec((pairs, rows, columns), lambda i, at: (0, 0, 0))] * 2,
    )
    return pl.pallas_call(
        latent_kernel,
        grid_spec=spec,
        out_shape=share_shapes(pairs, rows, columns),
        compiler_params=params(24),
        name="latent_attention",
    )(where, q, kv, words, wo)


def exchange(value, axis):
    return lax.all_to_all(value, axis, 0, 0, tiled=True)


def to_partner(value):
    count = lax.axis_size("head")
    return lax.ppermute(value, "head", [(i, i ^ 1) for i in range(count)])


def along_chips(value, distance):
    count = lax.axis_size("head")
    return lax.ppermute(
        value, "head", [(i, (i + 2 * distance) % count) for i in range(count)]
    )


def head_sum(where, own, theirs):
    kept, *sent = chip_sum(where, own, to_partner(theirs))
    return [kept] + [along_chips(value, d) for d, value in enumerate(sent, 1)]


def spread(pieces, seq_index):
    count = len(pieces)
    pair = pieces[count - 1]
    for k in range(count - 1):
        got = lax.ppermute(pieces[k], "seq", [(2 * count - 1, 2 * k + 1)])
        pair = jnp.where(seq_index == 2 * k + 1, got, pair)
    return pair


def pass_on(pair, seq_index, seq_count):
    passed = lax.ppermute(pair[0], "seq", [(k + 1, k) for k in range(0, seq_count, 2)])
    return jnp.where(seq_index % 2 == 0, passed, pair[1])


def per_device(
    context,
    wq_cross,
    wk_cross,
    wv_cross,
    wo_cross,
    wq_latent,
    wk_latent,
    wv_latent,
    wo_latent,
    cross_keep,
    latent_keep,
    residual_keep,
):
    seq_count = lax.axis_size("seq")
    head_count = lax.axis_size("head")
    root = seq_count - 1
    seq_index = lax.axis_index("seq").astype(jnp.int32)
    head_index = lax.axis_index("head").astype(jnp.int32)
    where = jnp.stack([seq_index, head_index])

    chunks = exchange(query_chunks(where, context, wq_cross, seq_count), "seq")
    keys, values = keys_values(context, wk_cross, wv_cross)
    rows, columns = chunks.shape[1:]
    held, keys = lax.optimization_barrier((context, keys))
    held = lax.dynamic_slice_in_dim(held, head_index * columns, columns, 1)
    held = held.reshape(seq_count // 2, 2, rows, columns)
    pieces = [held[k] for k in range(seq_count // 2)]
    own_queries, keys, values, *pieces = lax.optimization_barrier(
        (chunks[root], keys, values, *pieces)
    )
    queries = exchange(
        jnp.broadcast_to(own_queries[None], (seq_count, *own_queries.shape)), "seq"
    )
    queries, *pieces = lax.optimization_barrier((queries, *pieces))
    pair = spread(pieces, seq_index)
    parts = cross_attention(where, queries, keys, values, cross_keep, root)
    pair, parts = lax.optimization_barrier((pair, parts))
    parts = exchange(parts, "seq")
    inputs = pass_on(pair, seq_index, seq_count)
    parts, inputs = lax.optimization_barrier((parts, inputs))
    pairs = head_count // 2
    own, theirs = combine(where, parts, wo_cross, pairs)
    latents = residual(where, head_sum(where, own, theirs), inputs, residual_keep, 0)
    near = jnp.stack([latents] + [along_chips(latents, d) for d in range(1, pairs)])
    far = to_partner(near)
    q, kv = latent_qkv(where, near, far, wq_latent, wk_latent, wv_latent, seq_count)
    kv = exchange(kv, "seq")
    own, theirs = latent_attention(where, q, kv, latent_keep, wo_latent, pairs)
    return residual(where, head_sum(where, own, theirs), latents, residual_keep, 1)


def solution(mesh):
    in_specs = (
        P("seq", None),
        P(None, "head"),
        P(None, "head"),
        P(None, "head"),
        P("head", None),
        P(None, "head"),
        P(None, "head"),
        P(None, "head"),
        P("head", None),
        P("head", None, "seq"),
        P("head", None, None),
        P(),
    )
    out_specs = P("seq", "head")

    return jax.shard_map(
        per_device, mesh=mesh, in_specs=in_specs, out_specs=out_specs, check_vma=False
    )
```

```python
import math

import jax
import jax.numpy as jnp
from jax import lax
from jax.experimental import pallas as pl
from jax.experimental.pallas import tpu as pltpu
from jax.sharding import PartitionSpec as P


bf16 = jnp.bfloat16
f32 = jnp.float32
keep_scale = 8.0 / 7.0
masked = -1e30
head_dim = 128
query_scale = math.log2(math.e) / math.sqrt(head_dim)
stat_rows = 16
spread_size = 4


def params(limit=48):
    return pltpu.CompilerParams(
        dimension_semantics=("arbitrary",), vmem_limit_bytes=limit * 1024 * 1024
    )


def row_scale(rows):
    wide = rows.astype(f32)
    mean_square = jnp.mean(wide * wide, axis=-1, keepdims=True)
    return lax.rsqrt(mean_square + 1e-06)


def query_kernel(root, where_ref, x_ref, w_ref, out_ref):
    @pl.when(where_ref[0] == root)
    def _():
        x = x_ref[...]
        product = jnp.dot(x, w_ref[...], preferred_element_type=f32)
        out_ref[...] = (
            (product * (row_scale(x) * query_scale)).astype(bf16).reshape(out_ref.shape)
        )


def query_chunks(where, context, wq, seq_count):
    tok_rows, width = context.shape
    columns = wq.shape[1]
    rows = tok_rows // seq_count
    group = 4
    root = seq_count - 1
    spec = pltpu.PrefetchScalarGridSpec(
        num_scalar_prefetch=1,
        grid=(seq_count // group,),
        in_specs=[
            pl.BlockSpec((rows * group, width), lambda i, at: (jnp.where(at[0] == root, i, 0), 0)),
            pl.BlockSpec((width, columns), lambda i, at: (0, 0)),
        ],
        out_specs=pl.BlockSpec((group, rows, columns), lambda i, at: (i, 0, 0)),
    )
    return pl.pallas_call(
        lambda *refs: query_kernel(root, *refs),
        grid_spec=spec,
        out_shape=jax.ShapeDtypeStruct((seq_count, rows, columns), bf16),
        compiler_params=params(52),
        name="queries",
    )(where, context, wq)


def kv_kernel(x_ref, wk_ref, wv_ref, k_ref, v_ref):
    x = x_ref[...]
    scale = row_scale(x)
    k_ref[...] = (jnp.dot(x, wk_ref[...], preferred_element_type=f32) * scale).astype(bf16)
    v_ref[...] = (jnp.dot(x, wv_ref[...], preferred_element_type=f32) * scale).astype(bf16)


def keys_values(context, wk, wv):
    tok_rows, width = context.shape
    columns = wk.shape[1]
    block = 512
    return pl.pallas_call(
        kv_kernel,
        grid=(tok_rows // block,),
        in_specs=[
            pl.BlockSpec((block, width), lambda i: (i, 0)),
            pl.BlockSpec((width, columns), lambda i: (0, 0)),
            pl.BlockSpec((width, columns), lambda i: (0, 0)),
        ],
        out_specs=[pl.BlockSpec((block, columns), lambda i: (i, 0))] * 2,
        out_shape=[jax.ShapeDtypeStruct((tok_rows, columns), bf16)] * 2,
        compiler_params=params(52),
        name="keys_values",
    )(context, wk, wv)


def softmax_rows(scores_of, keep_of, values_of, pieces):
    scores = [scores_of(b) for b in range(pieces)]
    top = scores[0]
    for s in scores[1:]:
        top = jnp.maximum(top, s)
    top = jnp.max(top, axis=-1, keepdims=True)
    total = None
    summed = None
    for b in range(pieces):
        p = jnp.exp2(scores[b] - top)
        total = p if total is None else total + p
        kept = jnp.where(keep_of(b), p, 0.0).astype(bf16)
        part = jnp.dot(kept, values_of(b), preferred_element_type=f32)
        summed = part if summed is None else summed + part
    total = jnp.sum(total, axis=-1, keepdims=True)
    return summed, top, total


def nt_dot(a, b):
    return lax.dot_general(a, b, (((1,), (1,)), ((), ())), preferred_element_type=f32)


def cross_kernel(
    root, n, steps, where_ref, q_ref, k_ref, v_ref, words_ref, out_ref, s0_ref, s1_ref, m_ref
):
    rows = n * head_dim
    wide = words_ref.shape[2]
    step = pl.program_id(0)
    following = jnp.minimum(step + 1, steps - 1)

    def score(head, block, b, causal):
        cols = slice(head * head_dim, (head + 1) * head_dim)
        q = q_ref[pl.ds(block * n, n), :, cols].reshape(rows, head_dim)
        s = nt_dot(q, k_ref[b * wide : (b + 1) * wide, cols])
        if causal and (b + 1) * wide > block * rows:
            key = b * wide + lax.broadcasted_iota(jnp.int32, s.shape, 1)
            row = block * rows + lax.broadcasted_iota(jnp.int32, s.shape, 0)
            s = jnp.where(key <= row, s, masked)
        return s

    def stage(head, next_block, pieces, next_pieces, causal):
        ready, filling = (s0_ref, s1_ref) if head == 0 else (s1_ref, s0_ref)
        cols = slice(head * head_dim, (head + 1) * head_dim)
        words = words_ref[head].astype(jnp.int16)
        top = jnp.max(m_ref[head], axis=-1, keepdims=True)
        total = None
        summed = None
        next_top = None
        for b in range(max(pieces, next_pieces)):
            if b < next_pieces:
                s = score(1 - head, next_block, b, causal)
            if b < pieces:
                p = jnp.exp2(ready[b] - top)
                total = p if total is None else total + p
                kept = jnp.where(
                    (words & jnp.int16(1 << b)) != jnp.int16(0), p.astype(bf16), bf16(0)
                )
                part = jnp.dot(
                    kept, v_ref[b * wide : (b + 1) * wide, cols], preferred_element_type=f32
                )
                summed = part if summed is None else summed + part
            if b < next_pieces:
                filling[b] = s
                next_top = s if next_top is None else jnp.maximum(next_top, s)
        if next_pieces:
            m_ref[1 - head] = next_top
        total = jnp.sum(total, axis=-1, keepdims=True)
        out = (summed * (keep_scale / total)).astype(bf16)
        for i in range(n):
            out_ref[i, head * head_dim : (head + 1) * head_dim, :] = out[
                i * head_dim : (i + 1) * head_dim
            ]
        return top + jnp.log2(total)

    def first_scores(pieces, causal):
        first_top = None
        for b in range(pieces):
            s = score(0, 0, b, causal)
            s0_ref[b] = s
            first_top = s if first_top is None else jnp.maximum(first_top, s)
        m_ref[0] = first_top

    def run(block, next_block, pieces, next_pieces, causal):
        sums = [
            stage(0, block, pieces, pieces, causal),
            stage(1, next_block, pieces, next_pieces, causal),
        ]
        lanes = lax.broadcasted_iota(jnp.int32, (rows, head_dim), 1)
        stats = jnp.zeros((rows, head_dim), f32)
        for head, lse in enumerate(sums):
            high = lse.astype(bf16).astype(f32)
            middle = (lse - high).astype(bf16).astype(f32)
            low = lse - high - middle
            for j, piece in enumerate((high, middle, low)):
                stats = jnp.where(lanes == head * 3 + j, piece, stats)
        for i in range(n):
            out_ref[i, 2 * head_dim :, :] = (
                stats[i * head_dim : (i + 1) * head_dim].T[:stat_rows].astype(bf16)
            )

    for k in range(steps):

        @pl.when((where_ref[0] == root) & (step == k))
        def _():
            reach = [(j + 1) * rows // wide for j in range(steps)] + [0]
            if k == 0:
                first_scores(reach[0], True)
            run(k, k + 1, reach[k], reach[k + 1], True)

    @pl.when(where_ref[0] != root)
    def _():
        @pl.when(step == 0)
        def _():
            first_scores(8, False)

        run(step, following, 8, 8, False)


def cross_attention(where, queries, keys, values, words, root):
    count = queries.shape[0]
    n = 4
    rows = n * head_dim
    wide = words.shape[2]
    whole = pl.Buffered(1)
    spec = pltpu.PrefetchScalarGridSpec(
        num_scalar_prefetch=1,
        grid=(count // n,),
        in_specs=[
            pl.BlockSpec(queries.shape, lambda i, at: (0, 0, 0), pipeline_mode=whole),
            pl.BlockSpec(keys.shape, lambda i, at: (0, 0), pipeline_mode=whole),
            pl.BlockSpec(values.shape, lambda i, at: (0, 0), pipeline_mode=whole),
            pl.BlockSpec((2, rows, wide), lambda i, at: (0, i, 0)),
        ],
        out_specs=pl.BlockSpec((n, 2 * head_dim + stat_rows, head_dim), lambda i, at: (i, 0, 0)),
        scratch_shapes=[
            pltpu.VMEM((8, rows, wide), f32),
            pltpu.VMEM((8, rows, wide), f32),
            pltpu.VMEM((2, rows, wide), f32),
        ],
    )
    return pl.pallas_call(
        lambda *refs: cross_kernel(root, n, count // n, *refs),
        grid_spec=spec,
        out_shape=jax.ShapeDtypeStruct((count, 2 * head_dim + stat_rows, head_dim), bf16),
        compiler_params=params(52),
        cost_estimate=pl.CostEstimate(
            flops=8 * count * head_dim * keys.shape[0] * head_dim,
            transcendentals=2 * count * head_dim * keys.shape[0],
            bytes_accessed=4 * words.size,
        ),
        name="cross_attention",
    )(where, queries, keys, values, words)


def project_shares(attended, wo_ref, core, own_ref, theirs_ref):
    columns = own_ref.shape[2]
    for p in range(own_ref.shape[0]):
        for side, out_ref in ((core, own_ref), (1 - core, theirs_ref)):
            first = pl.multiple_of((2 * p + side) * columns, columns)
            share = jnp.dot(
                attended, wo_ref[:, pl.ds(first, columns)], preferred_element_type=f32
            )
            out_ref[p] = share.astype(out_ref.dtype)


def share_shapes(pairs, rows, columns):
    return [
        jax.ShapeDtypeStruct((pairs, rows, columns), f32),
        jax.ShapeDtypeStruct((pairs, rows, columns), bf16),
    ]


def combine_kernel(where_ref, parts_ref, wo_hbm, own_ref, theirs_ref, wo_ref, sem):
    fetch = pltpu.make_async_copy(wo_hbm, wo_ref, sem)
    fetch.start()
    count = parts_ref.shape[0]
    rows = head_dim
    heads = []
    stats = parts_ref[:, 2 * rows :, :].astype(f32)
    for head in range(2):
        lse = stats[:, head * 3] + stats[:, head * 3 + 1] + stats[:, head * 3 + 2]
        weight = jnp.exp2(lse - jnp.max(lse, axis=0, keepdims=True))
        weight = weight / jnp.sum(weight, axis=0, keepdims=True)
        weight = jnp.concatenate([weight, jnp.zeros((rows - count, rows), f32)], axis=0).T
        mixed = None
        for s in range(count):
            part = parts_ref[s, head * rows : (head + 1) * rows, :].astype(f32)
            part = part * weight[:, s : s + 1]
            mixed = part if mixed is None else mixed + part
        heads.append(mixed.astype(bf16))
    attended = jnp.concatenate(heads, axis=1)
    fetch.wait()
    project_shares(attended, wo_ref, where_ref[1] % 2, own_ref, theirs_ref)


def combine(where, parts, wo, pairs):
    whole = lambda i, at: (0, 0, 0)
    spec = pltpu.PrefetchScalarGridSpec(
        num_scalar_prefetch=1,
        grid=(1,),
        in_specs=[
            pl.BlockSpec(parts.shape, whole),
            pl.BlockSpec(memory_space=pltpu.HBM),
        ],
        out_specs=[pl.BlockSpec((pairs, head_dim, 256), whole)] * 2,
        scratch_shapes=[pltpu.VMEM(wo.shape, bf16), pltpu.SemaphoreType.DMA(())],
    )
    return pl.pallas_call(
        combine_kernel,
        grid_spec=spec,
        out_shape=share_shapes(pairs, head_dim, 256),
        compiler_params=params(16),
        name="combine",
    )(where, parts, pltpu.with_memory_space_constraint(wo, pltpu.HBM))


def chip_sum_kernel(where_ref, own_ref, got_ref, kept_ref, *out_refs):
    pairs = own_ref.shape[0]
    place = where_ref[1] // 2
    kept_ref[...] = own_ref[place] + got_ref[place].astype(f32)
    for d, out_ref in enumerate(out_refs, 1):
        target = lax.rem(place + d, pairs)
        out_ref[...] = (own_ref[target] + got_ref[target].astype(f32)).astype(bf16)


def chip_sum(where, own, got):
    pairs, rows, columns = own.shape
    flat = lambda i, at: (0, 0)
    spec = pltpu.PrefetchScalarGridSpec(
        num_scalar_prefetch=1,
        grid=(1,),
        in_specs=[pl.BlockSpec(own.shape, lambda i, at: (0, 0, 0))] * 2,
        out_specs=[pl.BlockSpec((rows, columns), flat)] * pairs,
    )
    return pl.pallas_call(
        chip_sum_kernel,
        grid_spec=spec,
        out_shape=[jax.ShapeDtypeStruct((rows, columns), f32)]
        + [jax.ShapeDtypeStruct((rows, columns), bf16)] * (pairs - 1),
        compiler_params=params(8),
        name="chip_sum",
    )(where, own, got)


def residual_kernel(where_ref, *refs):
    *share_refs, base_ref, words_ref, out_ref = refs
    total = share_refs[0][...].astype(f32)
    for ref in share_refs[1:]:
        total = total + ref[...].astype(f32)
    words = words_ref[0]
    for half in range(2):
        cols = slice(half * 128, half * 128 + 128)
        flag = (jnp.right_shift(words, where_ref[1] * 2 + half) & 1).astype(f32)
        base = base_ref[:, cols].astype(f32)
        out_ref[:, cols] = (base + flag * keep_scale * total[:, cols]).astype(bf16)


def residual(where, shares, base, words, index):
    rows, columns = base.shape
    flat = lambda i, at: (0, 0)
    spec = pltpu.PrefetchScalarGridSpec(
        num_scalar_prefetch=1,
        grid=(1,),
        in_specs=[pl.BlockSpec((rows, columns), flat)] * (len(shares) + 1)
        + [pl.BlockSpec((1, rows, 128), lambda i, at: (index, at[0], 0))],
        out_specs=pl.BlockSpec((rows, columns), flat),
    )
    return pl.pallas_call(
        residual_kernel,
        grid_spec=spec,
        out_shape=jax.ShapeDtypeStruct((rows, columns), bf16),
        compiler_params=params(8),
        name="residual",
    )(where, *shares, base, words)


def latent_qkv_kernel(where_ref, near_ref, far_ref, wq_ref, wk_ref, wv_ref, q_ref, kv_ref):
    pairs, _, columns = near_ref.shape
    place = where_ref[1] // 2
    core = where_ref[1] % 2
    pieces = []
    for d in range(pairs):
        chip = lax.rem(place + pairs - d, pairs)
        for ref, side in ((near_ref, core), (far_ref, 1 - core)):
            first = pl.multiple_of((2 * chip + side) * columns, columns)
            pieces.append((ref[d], first))
    squares = None
    for piece, _ in pieces:
        wide = piece.astype(f32)
        part = jnp.sum(wide * wide, axis=-1, keepdims=True)
        squares = part if squares is None else squares + part
    scale = lax.rsqrt(squares / (2 * pairs * columns) + 1e-06)

    def project(w_ref):
        total = None
        for piece, first in pieces:
            part = jnp.dot(piece, w_ref[pl.ds(first, columns), :], preferred_element_type=f32)
            total = part if total is None else total + part
        return total * scale

    q_ref[...] = (project(wq_ref) * query_scale).astype(bf16)
    keys = project(wk_ref).astype(bf16)
    values = project(wv_ref).astype(bf16)
    for s in range(kv_ref.shape[0]):
        kv_ref[s, :, :columns] = keys
        kv_ref[s, :, columns:] = values


def latent_qkv(where, near, far, wq, wk, wv, seq_count):
    _, rows, columns = near.shape
    spec = pltpu.PrefetchScalarGridSpec(
        num_scalar_prefetch=1,
        grid=(1,),
        in_specs=[pl.BlockSpec(near.shape, lambda i, at: (0, 0, 0))] * 2
        + [pl.BlockSpec(wq.shape, lambda i, at: (0, 0))] * 3,
        out_specs=[
            pl.BlockSpec((rows, columns), lambda i, at: (0, 0)),
            pl.BlockSpec((seq_count, rows, 2 * columns), lambda i, at: (0, 0, 0)),
        ],
    )
    return pl.pallas_call(
        latent_qkv_kernel,
        grid_spec=spec,
        out_shape=[
            jax.ShapeDtypeStruct((rows, columns), bf16),
            jax.ShapeDtypeStruct((seq_count, rows, 2 * columns), bf16),
        ],
        compiler_params=params(24),
        name="latent_qkv",
    )(where, near, far, wq, wk, wv)


def latent_kernel(where_ref, q_ref, kv_ref, words_ref, wo_ref, own_ref, theirs_ref):
    count, rows, _ = kv_ref.shape
    heads = []
    for head in range(2):
        cols = slice(head * head_dim, (head + 1) * head_dim)
        value_cols = slice(256 + head * head_dim, 256 + (head + 1) * head_dim)
        q = q_ref[:, cols]
        words = words_ref[head]

        def scores_of(t):
            s = nt_dot(q, kv_ref[t, :, cols])
            key = t * rows + lax.broadcasted_iota(jnp.int32, s.shape, 1)
            row = where_ref[0] * rows + lax.broadcasted_iota(jnp.int32, s.shape, 0)
            return jnp.where(key <= row, s, masked)

        summed, _, total = softmax_rows(
            scores_of,
            lambda t: (words & (1 << t)) != 0,
            lambda t: kv_ref[t, :, value_cols],
            count,
        )
        heads.append((summed * (keep_scale / total)).astype(bf16))
    attended = jnp.concatenate(heads, axis=1)
    project_shares(attended, wo_ref, where_ref[1] % 2, own_ref, theirs_ref)


def latent_attention(where, q, kv, words, wo, pairs):
    rows, columns = q.shape
    spec = pltpu.PrefetchScalarGridSpec(
        num_scalar_prefetch=1,
        grid=(1,),
        in_specs=[
            pl.BlockSpec(q.shape, lambda i, at: (0, 0)),
            pl.BlockSpec(kv.shape, lambda i, at: (0, 0, 0)),
            pl.BlockSpec((2, rows, 128), lambda i, at: (0, at[0], 0)),
            pl.BlockSpec(wo.shape, lambda i, at: (0, 0)),
        ],
        out_specs=[pl.BlockSpec((pairs, rows, columns), lambda i, at: (0, 0, 0))] * 2,
    )
    return pl.pallas_call(
        latent_kernel,
        grid_spec=spec,
        out_shape=share_shapes(pairs, rows, columns),
        compiler_params=params(24),
        name="latent_attention",
    )(where, q, kv, words, wo)


def exchange(value, axis):
    return lax.all_to_all(value, axis, 0, 0, tiled=True)


def to_partner(value):
    count = lax.axis_size("head")
    return lax.ppermute(value, "head", [(i, i ^ 1) for i in range(count)])


def along_chips(value, distance):
    count = lax.axis_size("head")
    return lax.ppermute(
        value, "head", [(i, (i + 2 * distance) % count) for i in range(count)]
    )


def head_sum(where, own, theirs):
    kept, *sent = chip_sum(where, own, to_partner(theirs))
    return [kept] + [along_chips(value, d) for d, value in enumerate(sent, 1)]


def spread(pieces, seq_index):
    count = len(pieces)
    quad = pieces[count - 1]
    size = quad.shape[0]
    for k in range(count - 1):
        owner = (k + 1) * size - 1
        got = lax.ppermute(pieces[k], "seq", [(count * size - 1, owner)])
        quad = jnp.where(seq_index == owner, got, quad)
    return quad


def pass_on(quad, seq_index, seq_count):
    size = quad.shape[0]
    mine = quad[size - 1]
    for j in range(size - 1):
        pairs = [(k + size - 1, k + j) for k in range(0, seq_count, size)]
        got = lax.ppermute(quad[j], "seq", pairs)
        mine = jnp.where(seq_index % size == j, got, mine)
    return mine


def per_device(
    context,
    wq_cross,
    wk_cross,
    wv_cross,
    wo_cross,
    wq_latent,
    wk_latent,
    wv_latent,
    wo_latent,
    cross_keep,
    latent_keep,
    residual_keep,
):
    seq_count = lax.axis_size("seq")
    head_count = lax.axis_size("head")
    root = seq_count - 1
    seq_index = lax.axis_index("seq").astype(jnp.int32)
    head_index = lax.axis_index("head").astype(jnp.int32)
    where = jnp.stack([seq_index, head_index])

    chunks = exchange(query_chunks(where, context, wq_cross, seq_count), "seq")
    keys, values = keys_values(context, wk_cross, wv_cross)
    rows, columns = chunks.shape[1:]
    held, keys = lax.optimization_barrier((context, keys))
    held = lax.dynamic_slice_in_dim(held, head_index * columns, columns, 1)
    held = held.reshape(seq_count // spread_size, spread_size, rows, columns)
    pieces = [held[k] for k in range(seq_count // spread_size)]
    own_queries, keys, values, *pieces = lax.optimization_barrier(
        (chunks[root], keys, values, *pieces)
    )
    queries = exchange(
        jnp.broadcast_to(own_queries[None], (seq_count, *own_queries.shape)), "seq"
    )
    queries, *pieces = lax.optimization_barrier((queries, *pieces))
    pair = spread(pieces, seq_index)
    parts = cross_attention(where, queries, keys, values, cross_keep, root)
    pair, parts = lax.optimization_barrier((pair, parts))
    parts = exchange(parts, "seq")
    inputs = pass_on(pair, seq_index, seq_count)
    parts, inputs = lax.optimization_barrier((parts, inputs))
    pairs = head_count // 2
    own, theirs = combine(where, parts, wo_cross, pairs)
    latents = residual(where, head_sum(where, own, theirs), inputs, residual_keep, 0)
    near = jnp.stack([latents] + [along_chips(latents, d) for d in range(1, pairs)])
    far = to_partner(near)
    q, kv = latent_qkv(where, near, far, wq_latent, wk_latent, wv_latent, seq_count)
    kv = exchange(kv, "seq")
    own, theirs = latent_attention(where, q, kv, latent_keep, wo_latent, pairs)
    return residual(where, head_sum(where, own, theirs), latents, residual_keep, 1)


def solution(mesh):
    in_specs = (
        P("seq", None),
        P(None, "head"),
        P(None, "head"),
        P(None, "head"),
        P("head", None),
        P(None, "head"),
        P(None, "head"),
        P(None, "head"),
        P("head", None),
        P("head", None, "seq"),
        P("head", None, None),
        P(),
    )
    out_specs = P("seq", "head")

    return jax.shard_map(
        per_device, mesh=mesh, in_specs=in_specs, out_specs=out_specs, check_vma=False
    )
```

```python
import math

import jax
import jax.numpy as jnp
from jax import lax
from jax.experimental import pallas as pl
from jax.experimental.pallas import tpu as pltpu
from jax.sharding import PartitionSpec as P


bf16 = jnp.bfloat16
f32 = jnp.float32
keep_scale = 8.0 / 7.0
masked = -1e30
head_dim = 128
query_scale = math.log2(math.e) / math.sqrt(head_dim)
stat_rows = 16
spread_size = 4


def params(limit=48):
    return pltpu.CompilerParams(
        dimension_semantics=("arbitrary",), vmem_limit_bytes=limit * 1024 * 1024
    )


def row_scale(rows):
    wide = rows.astype(f32)
    mean_square = jnp.mean(wide * wide, axis=-1, keepdims=True)
    return lax.rsqrt(mean_square + 1e-06)


def query_kernel(root, where_ref, x_ref, w_ref, out_ref):
    @pl.when(where_ref[0] == root)
    def _():
        x = x_ref[...]
        product = jnp.dot(x, w_ref[...], preferred_element_type=f32)
        out_ref[...] = (
            (product * (row_scale(x) * query_scale)).astype(bf16).reshape(out_ref.shape)
        )


def query_chunks(where, context, wq, seq_count):
    tok_rows, width = context.shape
    columns = wq.shape[1]
    rows = tok_rows // seq_count
    group = 4
    root = seq_count - 1
    spec = pltpu.PrefetchScalarGridSpec(
        num_scalar_prefetch=1,
        grid=(seq_count // group,),
        in_specs=[
            pl.BlockSpec((rows * group, width), lambda i, at: (jnp.where(at[0] == root, i, 0), 0)),
            pl.BlockSpec((width, columns), lambda i, at: (0, 0)),
        ],
        out_specs=pl.BlockSpec((group, rows, columns), lambda i, at: (i, 0, 0)),
    )
    return pl.pallas_call(
        lambda *refs: query_kernel(root, *refs),
        grid_spec=spec,
        out_shape=jax.ShapeDtypeStruct((seq_count, rows, columns), bf16),
        compiler_params=params(52),
        name="queries",
    )(where, context, wq)


def kv_kernel(x_ref, wk_ref, wv_ref, k_ref, v_ref):
    x = x_ref[...]
    scale = row_scale(x)
    k_ref[...] = (jnp.dot(x, wk_ref[...], preferred_element_type=f32) * scale).astype(bf16)
    v_ref[...] = (jnp.dot(x, wv_ref[...], preferred_element_type=f32) * scale).astype(bf16)


def keys_values(context, wk, wv):
    tok_rows, width = context.shape
    columns = wk.shape[1]
    block = 512
    return pl.pallas_call(
        kv_kernel,
        grid=(tok_rows // block,),
        in_specs=[
            pl.BlockSpec((block, width), lambda i: (i, 0)),
            pl.BlockSpec((width, columns), lambda i: (0, 0)),
            pl.BlockSpec((width, columns), lambda i: (0, 0)),
        ],
        out_specs=[pl.BlockSpec((block, columns), lambda i: (i, 0))] * 2,
        out_shape=[jax.ShapeDtypeStruct((tok_rows, columns), bf16)] * 2,
        compiler_params=params(52),
        name="keys_values",
    )(context, wk, wv)


def softmax_rows(scores_of, keep_of, values_of, pieces):
    scores = [scores_of(b) for b in range(pieces)]
    top = scores[0]
    for s in scores[1:]:
        top = jnp.maximum(top, s)
    top = jnp.max(top, axis=-1, keepdims=True)
    total = None
    summed = None
    for b in range(pieces):
        p = jnp.exp2(scores[b] - top)
        total = p if total is None else total + p
        kept = jnp.where(keep_of(b), p, 0.0).astype(bf16)
        part = jnp.dot(kept, values_of(b), preferred_element_type=f32)
        summed = part if summed is None else summed + part
    total = jnp.sum(total, axis=-1, keepdims=True)
    return summed, top, total


def nt_dot(a, b):
    return lax.dot_general(a, b, (((1,), (1,)), ((), ())), preferred_element_type=f32)


def cross_kernel(
    root, n, steps, where_ref, q_ref, k_ref, v_ref, words_ref, out_ref, s0_ref, s1_ref, m_ref
):
    rows = n * head_dim
    wide = words_ref.shape[2]
    step = pl.program_id(0)
    following = jnp.minimum(step + 1, steps - 1)

    def score(head, block, b, causal):
        cols = slice(head * head_dim, (head + 1) * head_dim)
        q = q_ref[pl.ds(block * n, n), :, cols].reshape(rows, head_dim)
        s = nt_dot(q, k_ref[b * wide : (b + 1) * wide, cols])
        if causal and (b + 1) * wide > block * rows:
            key = b * wide + lax.broadcasted_iota(jnp.int32, s.shape, 1)
            row = block * rows + lax.broadcasted_iota(jnp.int32, s.shape, 0)
            s = jnp.where(key <= row, s, masked)
        return s

    def stage(head, next_block, pieces, next_pieces, causal):
        ready, filling = (s0_ref, s1_ref) if head == 0 else (s1_ref, s0_ref)
        cols = slice(head * head_dim, (head + 1) * head_dim)
        words = words_ref[head].astype(jnp.int16)
        top = jnp.max(m_ref[head], axis=-1, keepdims=True)
        total = None
        summed = None
        next_top = None
        for b in range(max(pieces, next_pieces)):
            if b < next_pieces:
                s = score(1 - head, next_block, b, causal)
            if b < pieces:
                p = jnp.exp2(ready[b] - top)
                total = p if total is None else total + p
                kept = jnp.where(
                    (words & jnp.int16(1 << b)) != jnp.int16(0), p.astype(bf16), bf16(0)
                )
                part = jnp.dot(
                    kept, v_ref[b * wide : (b + 1) * wide, cols], preferred_element_type=f32
                )
                summed = part if summed is None else summed + part
            if b < next_pieces:
                filling[b] = s
                next_top = s if next_top is None else jnp.maximum(next_top, s)
        if next_pieces:
            m_ref[1 - head] = next_top
        total = jnp.sum(total, axis=-1, keepdims=True)
        out = (summed * (keep_scale / total)).astype(bf16)
        for i in range(n):
            out_ref[i, head * head_dim : (head + 1) * head_dim, :] = out[
                i * head_dim : (i + 1) * head_dim
            ]
        return top + jnp.log2(total)

    def first_scores(pieces, causal):
        first_top = None
        for b in range(pieces):
            s = score(0, 0, b, causal)
            s0_ref[b] = s
            first_top = s if first_top is None else jnp.maximum(first_top, s)
        m_ref[0] = first_top

    def run(block, next_block, pieces, next_pieces, causal):
        sums = [
            stage(0, block, pieces, pieces, causal),
            stage(1, next_block, pieces, next_pieces, causal),
        ]
        lanes = lax.broadcasted_iota(jnp.int32, (rows, head_dim), 1)
        stats = jnp.zeros((rows, head_dim), f32)
        for head, lse in enumerate(sums):
            high = lse.astype(bf16).astype(f32)
            middle = (lse - high).astype(bf16).astype(f32)
            low = lse - high - middle
            for j, piece in enumerate((high, middle, low)):
                stats = jnp.where(lanes == head * 3 + j, piece, stats)
        for i in range(n):
            out_ref[i, 2 * head_dim :, :] = (
                stats[i * head_dim : (i + 1) * head_dim].T[:stat_rows].astype(bf16)
            )

    for k in range(steps):

        @pl.when((where_ref[0] == root) & (step == k))
        def _():
            reach = [(j + 1) * rows // wide for j in range(steps)] + [0]
            if k == 0:
                first_scores(reach[0], True)
            run(k, k + 1, reach[k], reach[k + 1], True)

    @pl.when(where_ref[0] != root)
    def _():
        @pl.when(step == 0)
        def _():
            first_scores(8, False)

        run(step, following, 8, 8, False)


def cross_attention(where, queries, keys, values, words, root):
    count = queries.shape[0]
    n = 4
    rows = n * head_dim
    wide = words.shape[2]
    whole = pl.Buffered(1)
    spec = pltpu.PrefetchScalarGridSpec(
        num_scalar_prefetch=1,
        grid=(count // n,),
        in_specs=[
            pl.BlockSpec(queries.shape, lambda i, at: (0, 0, 0), pipeline_mode=whole),
            pl.BlockSpec(keys.shape, lambda i, at: (0, 0), pipeline_mode=whole),
            pl.BlockSpec(values.shape, lambda i, at: (0, 0), pipeline_mode=whole),
            pl.BlockSpec((2, rows, wide), lambda i, at: (0, i, 0)),
        ],
        out_specs=pl.BlockSpec((n, 2 * head_dim + stat_rows, head_dim), lambda i, at: (i, 0, 0)),
        scratch_shapes=[
            pltpu.VMEM((8, rows, wide), f32),
            pltpu.VMEM((8, rows, wide), f32),
            pltpu.VMEM((2, rows, wide), f32),
        ],
    )
    return pl.pallas_call(
        lambda *refs: cross_kernel(root, n, count // n, *refs),
        grid_spec=spec,
        out_shape=jax.ShapeDtypeStruct((count, 2 * head_dim + stat_rows, head_dim), bf16),
        compiler_params=params(52),
        cost_estimate=pl.CostEstimate(
            flops=8 * count * head_dim * keys.shape[0] * head_dim,
            transcendentals=2 * count * head_dim * keys.shape[0],
            bytes_accessed=4 * words.size,
        ),
        name="cross_attention",
    )(where, queries, keys, values, words)


def project_shares(attended, wo_ref, core, own_ref, theirs_ref):
    columns = own_ref.shape[2]
    for p in range(own_ref.shape[0]):
        for side, out_ref in ((core, own_ref), (1 - core, theirs_ref)):
            first = pl.multiple_of((2 * p + side) * columns, columns)
            share = jnp.dot(
                attended, wo_ref[:, pl.ds(first, columns)], preferred_element_type=f32
            )
            out_ref[p] = share.astype(out_ref.dtype)


def share_shapes(pairs, rows, columns):
    return [
        jax.ShapeDtypeStruct((pairs, rows, columns), f32),
        jax.ShapeDtypeStruct((pairs, rows, columns), bf16),
    ]


def combine_kernel(where_ref, parts_ref, wo_hbm, own_ref, theirs_ref, wo_ref, sem):
    fetch = pltpu.make_async_copy(wo_hbm, wo_ref, sem)
    fetch.start()
    count = parts_ref.shape[0]
    rows = head_dim
    heads = []
    stats = parts_ref[:, 2 * rows :, :].astype(f32)
    for head in range(2):
        lse = stats[:, head * 3] + stats[:, head * 3 + 1] + stats[:, head * 3 + 2]
        weight = jnp.exp2(lse - jnp.max(lse, axis=0, keepdims=True))
        weight = weight / jnp.sum(weight, axis=0, keepdims=True)
        weight = jnp.concatenate([weight, jnp.zeros((rows - count, rows), f32)], axis=0).T
        mixed = None
        for s in range(count):
            part = parts_ref[s, head * rows : (head + 1) * rows, :].astype(f32)
            part = part * weight[:, s : s + 1]
            mixed = part if mixed is None else mixed + part
        heads.append(mixed.astype(bf16))
    attended = jnp.concatenate(heads, axis=1)
    fetch.wait()
    project_shares(attended, wo_ref, where_ref[1] % 2, own_ref, theirs_ref)


def combine(where, parts, wo, pairs):
    whole = lambda i, at: (0, 0, 0)
    spec = pltpu.PrefetchScalarGridSpec(
        num_scalar_prefetch=1,
        grid=(1,),
        in_specs=[
            pl.BlockSpec(parts.shape, whole),
            pl.BlockSpec(memory_space=pltpu.HBM),
        ],
        out_specs=[pl.BlockSpec((pairs, head_dim, 256), whole)] * 2,
        scratch_shapes=[pltpu.VMEM(wo.shape, bf16), pltpu.SemaphoreType.DMA(())],
    )
    return pl.pallas_call(
        combine_kernel,
        grid_spec=spec,
        out_shape=share_shapes(pairs, head_dim, 256),
        compiler_params=params(16),
        name="combine",
    )(where, parts, pltpu.with_memory_space_constraint(wo, pltpu.HBM))


def chip_sum_kernel(where_ref, own_ref, got_ref, kept_ref, *out_refs):
    pairs = own_ref.shape[0]
    place = where_ref[1] // 2
    kept_ref[...] = own_ref[place] + got_ref[place].astype(f32)
    for d, out_ref in enumerate(out_refs, 1):
        target = lax.rem(place + d, pairs)
        out_ref[...] = (own_ref[target] + got_ref[target].astype(f32)).astype(bf16)


def chip_sum(where, own, got):
    pairs, rows, columns = own.shape
    flat = lambda i, at: (0, 0)
    spec = pltpu.PrefetchScalarGridSpec(
        num_scalar_prefetch=1,
        grid=(1,),
        in_specs=[pl.BlockSpec(own.shape, lambda i, at: (0, 0, 0))] * 2,
        out_specs=[pl.BlockSpec((rows, columns), flat)] * pairs,
    )
    return pl.pallas_call(
        chip_sum_kernel,
        grid_spec=spec,
        out_shape=[jax.ShapeDtypeStruct((rows, columns), f32)]
        + [jax.ShapeDtypeStruct((rows, columns), bf16)] * (pairs - 1),
        compiler_params=params(8),
        name="chip_sum",
    )(where, own, got)


def residual_kernel(where_ref, *refs):
    *share_refs, base_ref, words_ref, out_ref = refs
    total = share_refs[0][...].astype(f32)
    for ref in share_refs[1:]:
        total = total + ref[...].astype(f32)
    words = words_ref[0]
    for half in range(2):
        cols = slice(half * 128, half * 128 + 128)
        flag = (jnp.right_shift(words, where_ref[1] * 2 + half) & 1).astype(f32)
        base = base_ref[:, cols].astype(f32)
        out_ref[:, cols] = (base + flag * keep_scale * total[:, cols]).astype(bf16)


def residual(where, shares, base, words, index):
    rows, columns = base.shape
    flat = lambda i, at: (0, 0)
    spec = pltpu.PrefetchScalarGridSpec(
        num_scalar_prefetch=1,
        grid=(1,),
        in_specs=[pl.BlockSpec((rows, columns), flat)] * (len(shares) + 1)
        + [pl.BlockSpec((1, rows, 128), lambda i, at: (index, at[0], 0))],
        out_specs=pl.BlockSpec((rows, columns), flat),
    )
    return pl.pallas_call(
        residual_kernel,
        grid_spec=spec,
        out_shape=jax.ShapeDtypeStruct((rows, columns), bf16),
        compiler_params=params(8),
        name="residual",
    )(where, *shares, base, words)


def latent_qkv_kernel(where_ref, near_ref, far_ref, wq_ref, wk_ref, wv_ref, q_ref, kv_ref):
    pairs, _, columns = near_ref.shape
    place = where_ref[1] // 2
    core = where_ref[1] % 2
    pieces = []
    for d in range(pairs):
        chip = lax.rem(place + pairs - d, pairs)
        for ref, side in ((near_ref, core), (far_ref, 1 - core)):
            first = pl.multiple_of((2 * chip + side) * columns, columns)
            pieces.append((ref[d], first))
    squares = None
    for piece, _ in pieces:
        wide = piece.astype(f32)
        part = jnp.sum(wide * wide, axis=-1, keepdims=True)
        squares = part if squares is None else squares + part
    scale = lax.rsqrt(squares / (2 * pairs * columns) + 1e-06)

    def project(w_ref):
        total = None
        for piece, first in pieces:
            part = jnp.dot(piece, w_ref[pl.ds(first, columns), :], preferred_element_type=f32)
            total = part if total is None else total + part
        return total * scale

    q_ref[...] = (project(wq_ref) * query_scale).astype(bf16)
    keys = project(wk_ref).astype(bf16)
    values = project(wv_ref).astype(bf16)
    for s in range(kv_ref.shape[0]):
        kv_ref[s, :, :columns] = keys
        kv_ref[s, :, columns:] = values


def latent_qkv(where, near, far, wq, wk, wv, seq_count):
    _, rows, columns = near.shape
    spec = pltpu.PrefetchScalarGridSpec(
        num_scalar_prefetch=1,
        grid=(1,),
        in_specs=[pl.BlockSpec(near.shape, lambda i, at: (0, 0, 0))] * 2
        + [pl.BlockSpec(wq.shape, lambda i, at: (0, 0))] * 3,
        out_specs=[
            pl.BlockSpec((rows, columns), lambda i, at: (0, 0)),
            pl.BlockSpec((seq_count, rows, 2 * columns), lambda i, at: (0, 0, 0)),
        ],
    )
    return pl.pallas_call(
        latent_qkv_kernel,
        grid_spec=spec,
        out_shape=[
            jax.ShapeDtypeStruct((rows, columns), bf16),
            jax.ShapeDtypeStruct((seq_count, rows, 2 * columns), bf16),
        ],
        compiler_params=params(24),
        name="latent_qkv",
    )(where, near, far, wq, wk, wv)


def latent_kernel(where_ref, q_ref, kv_ref, words_ref, wo_ref, own_ref, theirs_ref):
    count, rows, _ = kv_ref.shape
    heads = []
    for head in range(2):
        cols = slice(head * head_dim, (head + 1) * head_dim)
        value_cols = slice(256 + head * head_dim, 256 + (head + 1) * head_dim)
        q = q_ref[:, cols]
        words = words_ref[head]

        def scores_of(t):
            s = nt_dot(q, kv_ref[t, :, cols])
            key = t * rows + lax.broadcasted_iota(jnp.int32, s.shape, 1)
            row = where_ref[0] * rows + lax.broadcasted_iota(jnp.int32, s.shape, 0)
            return jnp.where(key <= row, s, masked)

        summed, _, total = softmax_rows(
            scores_of,
            lambda t: (words & (1 << t)) != 0,
            lambda t: kv_ref[t, :, value_cols],
            count,
        )
        heads.append((summed * (keep_scale / total)).astype(bf16))
    attended = jnp.concatenate(heads, axis=1)
    project_shares(attended, wo_ref, where_ref[1] % 2, own_ref, theirs_ref)


def latent_attention(where, q, kv, words, wo, pairs):
    rows, columns = q.shape
    spec = pltpu.PrefetchScalarGridSpec(
        num_scalar_prefetch=1,
        grid=(1,),
        in_specs=[
            pl.BlockSpec(q.shape, lambda i, at: (0, 0)),
            pl.BlockSpec(kv.shape, lambda i, at: (0, 0, 0)),
            pl.BlockSpec((2, rows, 128), lambda i, at: (0, at[0], 0)),
            pl.BlockSpec(wo.shape, lambda i, at: (0, 0)),
        ],
        out_specs=[pl.BlockSpec((pairs, rows, columns), lambda i, at: (0, 0, 0))] * 2,
    )
    return pl.pallas_call(
        latent_kernel,
        grid_spec=spec,
        out_shape=share_shapes(pairs, rows, columns),
        compiler_params=params(24),
        name="latent_attention",
    )(where, q, kv, words, wo)


def exchange(value, axis):
    return lax.all_to_all(value, axis, 0, 0, tiled=True)


def to_partner(value):
    count = lax.axis_size("head")
    return lax.ppermute(value, "head", [(i, i ^ 1) for i in range(count)])


def along_chips(value, distance):
    count = lax.axis_size("head")
    return lax.ppermute(
        value, "head", [(i, (i + 2 * distance) % count) for i in range(count)]
    )


def head_sum(where, own, theirs, beside=()):
    kept, *sent = chip_sum(where, own, to_partner(theirs))
    *sent, beside = lax.optimization_barrier((*sent, list(beside)))
    return [kept] + [along_chips(value, d) for d, value in enumerate(sent, 1)], beside


def spread(pieces, seq_index):
    count = len(pieces)
    quad = pieces[count - 1]
    size = quad.shape[0]
    for k in range(count - 1):
        owner = (k + 1) * size - 1
        got = lax.ppermute(pieces[k], "seq", [(count * size - 1, owner)])
        quad = jnp.where(seq_index == owner, got, quad)
    return quad


def pass_on(slices, seq_index, seq_count):
    size = len(slices)
    mine = slices[size - 1]
    for j in range(size - 1):
        pairs = [(k + size - 1, k + j) for k in range(0, seq_count, size)]
        got = lax.ppermute(slices[j], "seq", pairs)
        mine = jnp.where(seq_index % size == j, got, mine)
    return mine


def per_device(
    context,
    wq_cross,
    wk_cross,
    wv_cross,
    wo_cross,
    wq_latent,
    wk_latent,
    wv_latent,
    wo_latent,
    cross_keep,
    latent_keep,
    residual_keep,
):
    seq_count = lax.axis_size("seq")
    head_count = lax.axis_size("head")
    root = seq_count - 1
    seq_index = lax.axis_index("seq").astype(jnp.int32)
    head_index = lax.axis_index("head").astype(jnp.int32)
    where = jnp.stack([seq_index, head_index])

    chunks = exchange(query_chunks(where, context, wq_cross, seq_count), "seq")
    keys, values = keys_values(context, wk_cross, wv_cross)
    rows, columns = chunks.shape[1:]
    held, keys = lax.optimization_barrier((context, keys))
    held = lax.dynamic_slice_in_dim(held, head_index * columns, columns, 1)
    held = held.reshape(seq_count // spread_size, spread_size, rows, columns)
    pieces = [held[k] for k in range(seq_count // spread_size)]
    own_queries, keys, values, *pieces = lax.optimization_barrier(
        (chunks[root], keys, values, *pieces)
    )
    queries = exchange(
        jnp.broadcast_to(own_queries[None], (seq_count, *own_queries.shape)), "seq"
    )
    queries, *pieces = lax.optimization_barrier((queries, *pieces))
    quad = spread(pieces, seq_index)
    parts = cross_attention(where, queries, keys, values, cross_keep, root)
    quad, parts = lax.optimization_barrier((quad, parts))
    parts = exchange(parts, "seq")
    pairs = head_count // 2
    own, theirs = combine(where, parts, wo_cross, pairs)
    slices = [quad[j] for j in range(spread_size)]
    shares, slices = head_sum(where, own, theirs, slices)
    inputs = pass_on(slices, seq_index, seq_count)
    latents = residual(where, shares, inputs, residual_keep, 0)
    near = jnp.stack([latents] + [along_chips(latents, d) for d in range(1, pairs)])
    far = to_partner(near)
    q, kv = latent_qkv(where, near, far, wq_latent, wk_latent, wv_latent, seq_count)
    kv = exchange(kv, "seq")
    own, theirs = latent_attention(where, q, kv, latent_keep, wo_latent, pairs)
    shares, _ = head_sum(where, own, theirs)
    return residual(where, shares, latents, residual_keep, 1)


def solution(mesh):
    in_specs = (
        P("seq", None),
        P(None, "head"),
        P(None, "head"),
        P(None, "head"),
        P("head", None),
        P(None, "head"),
        P(None, "head"),
        P(None, "head"),
        P("head", None),
        P("head", None, "seq"),
        P("head", None, None),
        P(),
    )
    out_specs = P("seq", "head")

    return jax.shard_map(
        per_device, mesh=mesh, in_specs=in_specs, out_specs=out_specs, check_vma=False
    )
```

```python
import math

import jax
import jax.numpy as jnp
from jax import lax
from jax.experimental import pallas as pl
from jax.experimental.pallas import tpu as pltpu
from jax.sharding import PartitionSpec as P


bf16 = jnp.bfloat16
f32 = jnp.float32
keep_scale = 8.0 / 7.0
masked = -1e30
head_dim = 128
query_scale = math.log2(math.e) / math.sqrt(head_dim)
stat_rows = 16
spread_size = 4


def params(limit=48):
    return pltpu.CompilerParams(
        dimension_semantics=("arbitrary",), vmem_limit_bytes=limit * 1024 * 1024
    )


def row_scale(rows):
    wide = rows.astype(f32)
    mean_square = jnp.mean(wide * wide, axis=-1, keepdims=True)
    return lax.rsqrt(mean_square + 1e-06)


def query_kernel(root, where_ref, x_ref, w_ref, out_ref):
    @pl.when(where_ref[0] == root)
    def _():
        x = x_ref[...]
        product = jnp.dot(x, w_ref[...], preferred_element_type=f32)
        out_ref[...] = (
            (product * (row_scale(x) * query_scale)).astype(bf16).reshape(out_ref.shape)
        )


def query_chunks(where, context, wq, seq_count):
    tok_rows, width = context.shape
    columns = wq.shape[1]
    rows = tok_rows // seq_count
    group = 4
    root = seq_count - 1
    spec = pltpu.PrefetchScalarGridSpec(
        num_scalar_prefetch=1,
        grid=(seq_count // group,),
        in_specs=[
            pl.BlockSpec((rows * group, width), lambda i, at: (jnp.where(at[0] == root, i, 0), 0)),
            pl.BlockSpec((width, columns), lambda i, at: (0, 0)),
        ],
        out_specs=pl.BlockSpec((group, rows, columns), lambda i, at: (i, 0, 0)),
    )
    return pl.pallas_call(
        lambda *refs: query_kernel(root, *refs),
        grid_spec=spec,
        out_shape=jax.ShapeDtypeStruct((seq_count, rows, columns), bf16),
        compiler_params=params(52),
        name="queries",
    )(where, context, wq)


def kv_kernel(x_ref, wk_ref, wv_ref, k_ref, v_ref):
    x = x_ref[...]
    scale = row_scale(x)
    k_ref[...] = (jnp.dot(x, wk_ref[...], preferred_element_type=f32) * scale).astype(bf16)
    v_ref[...] = (jnp.dot(x, wv_ref[...], preferred_element_type=f32) * scale).astype(bf16)


def keys_values(context, wk, wv):
    tok_rows, width = context.shape
    columns = wk.shape[1]
    block = 512
    return pl.pallas_call(
        kv_kernel,
        grid=(tok_rows // block,),
        in_specs=[
            pl.BlockSpec((block, width), lambda i: (i, 0)),
            pl.BlockSpec((width, columns), lambda i: (0, 0)),
            pl.BlockSpec((width, columns), lambda i: (0, 0)),
        ],
        out_specs=[pl.BlockSpec((block, columns), lambda i: (i, 0))] * 2,
        out_shape=[jax.ShapeDtypeStruct((tok_rows, columns), bf16)] * 2,
        compiler_params=params(52),
        name="keys_values",
    )(context, wk, wv)


def softmax_rows(scores_of, keep_of, values_of, pieces):
    scores = [scores_of(b) for b in range(pieces)]
    top = scores[0]
    for s in scores[1:]:
        top = jnp.maximum(top, s)
    top = jnp.max(top, axis=-1, keepdims=True)
    total = None
    summed = None
    for b in range(pieces):
        p = jnp.exp2(scores[b] - top)
        total = p if total is None else total + p
        kept = jnp.where(keep_of(b), p, 0.0).astype(bf16)
        part = jnp.dot(kept, values_of(b), preferred_element_type=f32)
        summed = part if summed is None else summed + part
    total = jnp.sum(total, axis=-1, keepdims=True)
    return summed, top, total


def nt_dot(a, b):
    return lax.dot_general(a, b, (((1,), (1,)), ((), ())), preferred_element_type=f32)


def cross_kernel(
    root, n, steps, where_ref, q_ref, k_ref, v_ref, words_ref, out_ref, s0_ref, s1_ref, m_ref
):
    rows = n * head_dim
    wide = words_ref.shape[2]
    step = pl.program_id(0)
    following = jnp.minimum(step + 1, steps - 1)

    def score(head, block, b, causal):
        cols = slice(head * head_dim, (head + 1) * head_dim)
        q = q_ref[pl.ds(block * n, n), :, cols].reshape(rows, head_dim)
        s = nt_dot(q, k_ref[b * wide : (b + 1) * wide, cols])
        if causal and (b + 1) * wide > block * rows:
            key = b * wide + lax.broadcasted_iota(jnp.int32, s.shape, 1)
            row = block * rows + lax.broadcasted_iota(jnp.int32, s.shape, 0)
            s = jnp.where(key <= row, s, masked)
        return s

    def stage(head, next_block, pieces, next_pieces, causal):
        ready, filling = (s0_ref, s1_ref) if head == 0 else (s1_ref, s0_ref)
        cols = slice(head * head_dim, (head + 1) * head_dim)
        words = words_ref[head].astype(jnp.int16)
        top = jnp.max(m_ref[head], axis=-1, keepdims=True)
        total = None
        summed = None
        next_top = None
        for b in range(max(pieces, next_pieces)):
            if b < next_pieces:
                s = score(1 - head, next_block, b, causal)
            if b < pieces:
                p = jnp.exp2(ready[b] - top)
                total = p if total is None else total + p
                kept = jnp.where(
                    (words & jnp.int16(1 << b)) != jnp.int16(0), p.astype(bf16), bf16(0)
                )
                part = jnp.dot(
                    kept, v_ref[b * wide : (b + 1) * wide, cols], preferred_element_type=f32
                )
                summed = part if summed is None else summed + part
            if b < next_pieces:
                filling[b] = s
                next_top = s if next_top is None else jnp.maximum(next_top, s)
        if next_pieces:
            m_ref[1 - head] = next_top
        total = jnp.sum(total, axis=-1, keepdims=True)
        out = (summed * (keep_scale / total)).astype(bf16)
        for i in range(n):
            out_ref[i, head * head_dim : (head + 1) * head_dim, :] = out[
                i * head_dim : (i + 1) * head_dim
            ]
        return top + jnp.log2(total)

    def first_scores(pieces, causal):
        first_top = None
        for b in range(pieces):
            s = score(0, 0, b, causal)
            s0_ref[b] = s
            first_top = s if first_top is None else jnp.maximum(first_top, s)
        m_ref[0] = first_top

    def run(block, next_block, pieces, next_pieces, causal):
        sums = [
            stage(0, block, pieces, pieces, causal),
            stage(1, next_block, pieces, next_pieces, causal),
        ]
        lanes = lax.broadcasted_iota(jnp.int32, (rows, head_dim), 1)
        stats = jnp.zeros((rows, head_dim), f32)
        for head, lse in enumerate(sums):
            high = lse.astype(bf16).astype(f32)
            middle = (lse - high).astype(bf16).astype(f32)
            low = lse - high - middle
            for j, piece in enumerate((high, middle, low)):
                stats = jnp.where(lanes == head * 3 + j, piece, stats)
        for i in range(n):
            out_ref[i, 2 * head_dim :, :] = (
                stats[i * head_dim : (i + 1) * head_dim].T[:stat_rows].astype(bf16)
            )

    for k in range(steps):

        @pl.when((where_ref[0] == root) & (step == k))
        def _():
            reach = [(j + 1) * rows // wide for j in range(steps)] + [0]
            if k == 0:
                first_scores(reach[0], True)
            run(k, k + 1, reach[k], reach[k + 1], True)

    @pl.when(where_ref[0] != root)
    def _():
        @pl.when(step == 0)
        def _():
            first_scores(8, False)

        run(step, following, 8, 8, False)


def cross_attention(where, queries, keys, values, words, root):
    count = queries.shape[0]
    n = 4
    rows = n * head_dim
    wide = words.shape[2]
    whole = pl.Buffered(1)
    spec = pltpu.PrefetchScalarGridSpec(
        num_scalar_prefetch=1,
        grid=(count // n,),
        in_specs=[
            pl.BlockSpec(queries.shape, lambda i, at: (0, 0, 0), pipeline_mode=whole),
            pl.BlockSpec(keys.shape, lambda i, at: (0, 0), pipeline_mode=whole),
            pl.BlockSpec(values.shape, lambda i, at: (0, 0), pipeline_mode=whole),
            pl.BlockSpec((2, rows, wide), lambda i, at: (0, i, 0)),
        ],
        out_specs=pl.BlockSpec((n, 2 * head_dim + stat_rows, head_dim), lambda i, at: (i, 0, 0)),
        scratch_shapes=[
            pltpu.VMEM((8, rows, wide), f32),
            pltpu.VMEM((8, rows, wide), f32),
            pltpu.VMEM((2, rows, wide), f32),
        ],
    )
    return pl.pallas_call(
        lambda *refs: cross_kernel(root, n, count // n, *refs),
        grid_spec=spec,
        out_shape=jax.ShapeDtypeStruct((count, 2 * head_dim + stat_rows, head_dim), bf16),
        compiler_params=params(52),
        cost_estimate=pl.CostEstimate(
            flops=8 * count * head_dim * keys.shape[0] * head_dim,
            transcendentals=2 * count * head_dim * keys.shape[0],
            bytes_accessed=4 * words.size,
        ),
        name="cross_attention",
    )(where, queries, keys, values, words)


def project_shares(attended, wo_ref, core, own_ref, theirs_ref):
    columns = own_ref.shape[2]
    for p in range(own_ref.shape[0]):
        for side, out_ref in ((core, own_ref), (1 - core, theirs_ref)):
            first = pl.multiple_of((2 * p + side) * columns, columns)
            share = jnp.dot(
                attended, wo_ref[:, pl.ds(first, columns)], preferred_element_type=f32
            )
            out_ref[p] = share.astype(out_ref.dtype)


def share_shapes(pairs, rows, columns):
    return [
        jax.ShapeDtypeStruct((pairs, rows, columns), f32),
        jax.ShapeDtypeStruct((pairs, rows, columns), bf16),
    ]


def combine_kernel(where_ref, parts_ref, wo_hbm, own_ref, theirs_ref, wo_ref, sem):
    fetch = pltpu.make_async_copy(wo_hbm, wo_ref, sem)
    fetch.start()
    count = parts_ref.shape[0]
    rows = head_dim
    heads = []
    stats = parts_ref[:, 2 * rows :, :].astype(f32)
    for head in range(2):
        lse = stats[:, head * 3] + stats[:, head * 3 + 1] + stats[:, head * 3 + 2]
        weight = jnp.exp2(lse - jnp.max(lse, axis=0, keepdims=True))
        weight = weight / jnp.sum(weight, axis=0, keepdims=True)
        weight = jnp.concatenate([weight, jnp.zeros((rows - count, rows), f32)], axis=0).T
        mixed = None
        for s in range(count):
            part = parts_ref[s, head * rows : (head + 1) * rows, :].astype(f32)
            part = part * weight[:, s : s + 1]
            mixed = part if mixed is None else mixed + part
        heads.append(mixed.astype(bf16))
    attended = jnp.concatenate(heads, axis=1)
    fetch.wait()
    project_shares(attended, wo_ref, where_ref[1] % 2, own_ref, theirs_ref)


def combine(where, parts, wo, pairs):
    whole = lambda i, at: (0, 0, 0)
    spec = pltpu.PrefetchScalarGridSpec(
        num_scalar_prefetch=1,
        grid=(1,),
        in_specs=[
            pl.BlockSpec(parts.shape, whole),
            pl.BlockSpec(memory_space=pltpu.HBM),
        ],
        out_specs=[pl.BlockSpec((pairs, head_dim, 256), whole)] * 2,
        scratch_shapes=[pltpu.VMEM(wo.shape, bf16), pltpu.SemaphoreType.DMA(())],
    )
    return pl.pallas_call(
        combine_kernel,
        grid_spec=spec,
        out_shape=share_shapes(pairs, head_dim, 256),
        compiler_params=params(16),
        name="combine",
    )(where, parts, pltpu.with_memory_space_constraint(wo, pltpu.HBM))


def chip_sum_kernel(where_ref, own_ref, got_ref, kept_ref, *out_refs):
    pairs = own_ref.shape[0]
    place = where_ref[1] // 2
    kept_ref[...] = own_ref[place] + got_ref[place].astype(f32)
    for d, out_ref in enumerate(out_refs, 1):
        target = lax.rem(place + d, pairs)
        out_ref[...] = (own_ref[target] + got_ref[target].astype(f32)).astype(bf16)


def chip_sum(where, own, got):
    pairs, rows, columns = own.shape
    flat = lambda i, at: (0, 0)
    spec = pltpu.PrefetchScalarGridSpec(
        num_scalar_prefetch=1,
        grid=(1,),
        in_specs=[pl.BlockSpec(own.shape, lambda i, at: (0, 0, 0))] * 2,
        out_specs=[pl.BlockSpec((rows, columns), flat)] * pairs,
    )
    return pl.pallas_call(
        chip_sum_kernel,
        grid_spec=spec,
        out_shape=[jax.ShapeDtypeStruct((rows, columns), f32)]
        + [jax.ShapeDtypeStruct((rows, columns), bf16)] * (pairs - 1),
        compiler_params=params(8),
        name="chip_sum",
    )(where, own, got)


def residual_kernel(where_ref, *refs):
    *share_refs, base_ref, words_ref, out_ref = refs
    total = share_refs[0][...].astype(f32)
    for ref in share_refs[1:]:
        total = total + ref[...].astype(f32)
    words = words_ref[0]
    for half in range(2):
        cols = slice(half * 128, half * 128 + 128)
        flag = (jnp.right_shift(words, where_ref[1] * 2 + half) & 1).astype(f32)
        base = base_ref[:, cols].astype(f32)
        out_ref[:, cols] = (base + flag * keep_scale * total[:, cols]).astype(bf16)


def residual(where, shares, base, words, index):
    rows, columns = base.shape
    flat = lambda i, at: (0, 0)
    spec = pltpu.PrefetchScalarGridSpec(
        num_scalar_prefetch=1,
        grid=(1,),
        in_specs=[pl.BlockSpec((rows, columns), flat)] * (len(shares) + 1)
        + [pl.BlockSpec((1, rows, 128), lambda i, at: (index, at[0], 0))],
        out_specs=pl.BlockSpec((rows, columns), flat),
    )
    return pl.pallas_call(
        residual_kernel,
        grid_spec=spec,
        out_shape=jax.ShapeDtypeStruct((rows, columns), bf16),
        compiler_params=params(8),
        name="residual",
    )(where, *shares, base, words)


def latent_qkv_kernel(where_ref, near_ref, far_ref, wq_ref, wk_ref, wv_ref, q_ref, kv_ref):
    pairs, _, columns = near_ref.shape
    place = where_ref[1] // 2
    core = where_ref[1] % 2
    pieces = []
    for d in range(pairs):
        chip = lax.rem(place + pairs - d, pairs)
        for ref, side in ((near_ref, core), (far_ref, 1 - core)):
            first = pl.multiple_of((2 * chip + side) * columns, columns)
            pieces.append((ref[d], first))
    squares = None
    for piece, _ in pieces:
        wide = piece.astype(f32)
        part = jnp.sum(wide * wide, axis=-1, keepdims=True)
        squares = part if squares is None else squares + part
    scale = lax.rsqrt(squares / (2 * pairs * columns) + 1e-06)

    def project(w_ref):
        total = None
        for piece, first in pieces:
            part = jnp.dot(piece, w_ref[pl.ds(first, columns), :], preferred_element_type=f32)
            total = part if total is None else total + part
        return total * scale

    q_ref[...] = (project(wq_ref) * query_scale).astype(bf16)
    keys = project(wk_ref).astype(bf16)
    values = project(wv_ref).astype(bf16)
    for s in range(kv_ref.shape[0]):
        kv_ref[s, :, :columns] = keys
        kv_ref[s, :, columns:] = values


def latent_qkv(where, near, far, wq, wk, wv, seq_count):
    _, rows, columns = near.shape
    spec = pltpu.PrefetchScalarGridSpec(
        num_scalar_prefetch=1,
        grid=(1,),
        in_specs=[pl.BlockSpec(near.shape, lambda i, at: (0, 0, 0))] * 2
        + [pl.BlockSpec(wq.shape, lambda i, at: (0, 0))] * 3,
        out_specs=[
            pl.BlockSpec((rows, columns), lambda i, at: (0, 0)),
            pl.BlockSpec((seq_count, rows, 2 * columns), lambda i, at: (0, 0, 0)),
        ],
    )
    return pl.pallas_call(
        latent_qkv_kernel,
        grid_spec=spec,
        out_shape=[
            jax.ShapeDtypeStruct((rows, columns), bf16),
            jax.ShapeDtypeStruct((seq_count, rows, 2 * columns), bf16),
        ],
        compiler_params=params(24),
        name="latent_qkv",
    )(where, near, far, wq, wk, wv)


def latent_kernel(where_ref, q_ref, kv_ref, words_ref, wo_ref, own_ref, theirs_ref):
    count, rows, _ = kv_ref.shape
    heads = []
    for head in range(2):
        cols = slice(head * head_dim, (head + 1) * head_dim)
        value_cols = slice(256 + head * head_dim, 256 + (head + 1) * head_dim)
        q = q_ref[:, cols]
        words = words_ref[head]

        def scores_of(t):
            s = nt_dot(q, kv_ref[t, :, cols])
            key = t * rows + lax.broadcasted_iota(jnp.int32, s.shape, 1)
            row = where_ref[0] * rows + lax.broadcasted_iota(jnp.int32, s.shape, 0)
            return jnp.where(key <= row, s, masked)

        summed, _, total = softmax_rows(
            scores_of,
            lambda t: (words & (1 << t)) != 0,
            lambda t: kv_ref[t, :, value_cols],
            count,
        )
        heads.append((summed * (keep_scale / total)).astype(bf16))
    attended = jnp.concatenate(heads, axis=1)
    project_shares(attended, wo_ref, where_ref[1] % 2, own_ref, theirs_ref)


def latent_attention(where, q, kv, words, wo, pairs):
    rows, columns = q.shape
    spec = pltpu.PrefetchScalarGridSpec(
        num_scalar_prefetch=1,
        grid=(1,),
        in_specs=[
            pl.BlockSpec(q.shape, lambda i, at: (0, 0)),
            pl.BlockSpec(kv.shape, lambda i, at: (0, 0, 0)),
            pl.BlockSpec((2, rows, 128), lambda i, at: (0, at[0], 0)),
            pl.BlockSpec(wo.shape, lambda i, at: (0, 0)),
        ],
        out_specs=[pl.BlockSpec((pairs, rows, columns), lambda i, at: (0, 0, 0))] * 2,
    )
    return pl.pallas_call(
        latent_kernel,
        grid_spec=spec,
        out_shape=share_shapes(pairs, rows, columns),
        compiler_params=params(24),
        name="latent_attention",
    )(where, q, kv, words, wo)


def exchange(value, axis):
    return lax.all_to_all(value, axis, 0, 0, tiled=True)


def to_partner(value):
    count = lax.axis_size("head")
    return lax.ppermute(value, "head", [(i, i ^ 1) for i in range(count)])


def along_chips(value, distance):
    count = lax.axis_size("head")
    return lax.ppermute(
        value, "head", [(i, (i + 2 * distance) % count) for i in range(count)]
    )


def head_sum(where, own, theirs):
    kept, *sent = chip_sum(where, own, to_partner(theirs))
    return [kept] + [along_chips(value, d) for d, value in enumerate(sent, 1)]


def spread(pieces, seq_index):
    count = len(pieces)
    quad = pieces[count - 1]
    size = quad.shape[0]
    for k in range(count - 1):
        owner = (k + 1) * size - 1
        got = lax.ppermute(pieces[k], "seq", [(count * size - 1, owner)])
        quad = jnp.where(seq_index == owner, got, quad)
    return quad


def pass_on(quad, seq_count):
    size = quad.shape[0]
    arrived = []
    for j in range(size - 1):
        pairs = [(k + size - 1, k + j) for k in range(0, seq_count, size)]
        arrived.append(lax.ppermute(quad[j], "seq", pairs))
    return arrived + [quad[size - 1]]


def choose(arrived, place):
    mine = arrived[-1]
    for j, got in enumerate(arrived[:-1]):
        mine = jnp.where(place == j, got, mine)
    return mine


def per_device(
    context,
    wq_cross,
    wk_cross,
    wv_cross,
    wo_cross,
    wq_latent,
    wk_latent,
    wv_latent,
    wo_latent,
    cross_keep,
    latent_keep,
    residual_keep,
):
    seq_count = lax.axis_size("seq")
    head_count = lax.axis_size("head")
    root = seq_count - 1
    seq_index = lax.axis_index("seq").astype(jnp.int32)
    head_index = lax.axis_index("head").astype(jnp.int32)
    where = jnp.stack([seq_index, head_index])

    chunks = exchange(query_chunks(where, context, wq_cross, seq_count), "seq")
    keys, values = keys_values(context, wk_cross, wv_cross)
    rows, columns = chunks.shape[1:]
    held, keys = lax.optimization_barrier((context, keys))
    held = lax.dynamic_slice_in_dim(held, head_index * columns, columns, 1)
    held = held.reshape(seq_count // spread_size, spread_size, rows, columns)
    pieces = [held[k] for k in range(seq_count // spread_size)]
    own_queries, keys, values, *pieces = lax.optimization_barrier(
        (chunks[root], keys, values, *pieces)
    )
    queries = exchange(
        jnp.broadcast_to(own_queries[None], (seq_count, *own_queries.shape)), "seq"
    )
    queries, *pieces = lax.optimization_barrier((queries, *pieces))
    pair = spread(pieces, seq_index)
    parts = cross_attention(where, queries, keys, values, cross_keep, root)
    pair, parts = lax.optimization_barrier((pair, parts))
    parts = exchange(parts, "seq")
    parts, *arrived = lax.optimization_barrier((parts, *pass_on(pair, seq_count)))
    pairs = head_count // 2
    own, theirs = combine(where, parts, wo_cross, pairs)
    theirs, *arrived = lax.optimization_barrier((theirs, *arrived))
    inputs = choose(arrived, seq_index % spread_size)
    latents = residual(where, head_sum(where, own, theirs), inputs, residual_keep, 0)
    near = jnp.stack([latents] + [along_chips(latents, d) for d in range(1, pairs)])
    far = to_partner(near)
    q, kv = latent_qkv(where, near, far, wq_latent, wk_latent, wv_latent, seq_count)
    kv = exchange(kv, "seq")
    own, theirs = latent_attention(where, q, kv, latent_keep, wo_latent, pairs)
    return residual(where, head_sum(where, own, theirs), latents, residual_keep, 1)


def solution(mesh):
    in_specs = (
        P("seq", None),
        P(None, "head"),
        P(None, "head"),
        P(None, "head"),
        P("head", None),
        P(None, "head"),
        P(None, "head"),
        P(None, "head"),
        P("head", None),
        P("head", None, "seq"),
        P("head", None, None),
        P(),
    )
    out_specs = P("seq", "head")

    return jax.shard_map(
        per_device, mesh=mesh, in_specs=in_specs, out_specs=out_specs, check_vma=False
    )
```
